32 devices in a mesh: hw: 8 (over y, x, core), head: 4 (over z).
Axes of the slice: x: 2, y: 2, z: 4, core: 2. Of those that a mesh axis runs over, the one named last changes fastest.
Arguments:
- latents: bfloat16 [8, 8, 8, 8, 5120], P('hw'), may hold values from -6 to 6
- query_weight: bfloat16 [5120, 2560], P('hw', 'head'), may hold values from -0.125 to 0.125
- key_weight: bfloat16 [5120, 2560], P('hw', 'head'), may hold values from -0.125 to 0.125
- value_weight: bfloat16 [5120, 2560], P('hw', 'head'), may hold values from -0.078125 to 0.078125
- output_weight: bfloat16 [2560, 5120], P('hw', 'head'), may hold values from -0.5 to 0.5
- query_gain: float32 [2560], P('head'), may hold values from 0.3 to 9
- key_gain: float32 [2560], P('head'), may hold values from 0.3 to 9
- frame_index: int32 [8], replicated, may hold values from 0 to 94, as said below
- row_index: int32 [32], replicated, may hold values from 0 to 286, as said below
- column_index: int32 [16], replicated, may hold values from 0 to 158, as said below
Outputs:
- attention_out: bfloat16 [8, 8, 8, 8, 5120], P('hw', None, None, None, 'head')
The draws below stay inside these ranges and needn't reach their ends.
Inputs may be any that keep to these rules, and one draw needn't show every extreme that they name: `frame_index`: strictly increasing. `row_index`: strictly increasing. `column_index`: strictly increasing.
All inputs are finite; a program needn't handle non-finite values.
Results may differ from the reference program's by a relative error of at most 0.0075.
The reference program's roundings to bfloat16 on the way count: a program that leaves them out, or rounds other values in their place, can miss the bound.
Values may be sent and summed in bfloat16 or wider, within the bound.
A program may use at most 128 MiB of HBM per device.

```python
import math
import jax
import jax.numpy as jnp
from jax import lax

D = 5120
HEADS = 20
HD = 128
WT = 4
DEV_ROWS = 4
FRAMES = 8
BS = 8
GRID_W = 2
BLOCKS = 8
HH = 32
WW = 16


def gain_values(key, salt):
    subkey = jax.random.fold_in(key, salt)
    return jnp.exp(jax.random.uniform(subkey, (HEADS * HD,), jnp.float32, -1.2, 1.2))


def position_values(key, salt, count):
    subkey = jax.random.fold_in(key, salt)
    top_stride = 30 // count + 8
    strides = jax.random.randint(subkey, (count,), 1, top_stride + 1, dtype=jnp.int32)
    total = jnp.sum(strides)
    most = jnp.int32(30 + 8 * count)
    return (most - (total - jnp.cumsum(strides))).astype(jnp.int32)


def draw_query_gain(key, part):
    return gain_values(key, 11)


def draw_key_gain(key, part):
    return gain_values(key, 12)


def draw_frame_index(key, part):
    return position_values(key, 21, FRAMES)


def draw_row_index(key, part):
    return position_values(key, 22, HH)


def draw_column_index(key, part):
    return position_values(key, 23, WW)


def strengthened(entries, key, source, target, blocks, factor):
    def block_of(position):
        return (jnp.arange(entries.shape[position]) // (entries.shape[position] // blocks)).reshape((-1,) + (1,) * (entries.ndim - 1 - position))

    near = jax.random.permutation(key, blocks)[block_of(target)]
    second = (block_of(target) + blocks // 2) % blocks
    return jnp.where((block_of(source) == near) | (block_of(source) == second), factor * entries, entries)


def level_of(stream_key, extent, shards, low, largest):
    def one(axis_at, parts):
        steps = jax.random.uniform(jax.random.fold_in(jax.random.fold_in(stream_key, 6), axis_at), (parts,), jnp.float32, low / len(shards), largest / len(shards))
        return jnp.repeat(jnp.exp(steps), extent[axis_at] // parts).reshape((-1,) + (1,) * (len(extent) - axis_at - 1))

    factor_of = one(*shards[0])
    for cut in shards[1:]:
        factor_of = factor_of * one(*cut)
    return factor_of


def normal_values(own_key, extent, deviation, reach, split=(), held_as=jnp.bfloat16):
    values = jax.random.normal(own_key, extent, jnp.float32) * deviation
    if len(split) > 0:
        values = level_of(own_key, extent, split, -0.22, 0.18) * values
    return jnp.clip(values, min=-reach, max=reach).astype(held_as)


def heavy_noise(rng, extent, deviation, most, shards, heavy, kind=jnp.bfloat16):
    values = deviation * jax.random.normal(rng, extent, jnp.float32)
    if shards:
        values = values * level_of(rng, extent, shards, -0.22, 0.18)
    return jnp.clip(strengthened(values, jax.random.fold_in(rng, 3), *heavy), -most, most).astype(kind)


def setup_inputs(seed: int = 0) -> dict:
    seeds = jax.random.split(jax.random.key(seed), 11)
    return {
        "latents": normal_values(seeds[0], (BLOCKS, FRAMES, BS, BS, D), 1.0, 6.0, ((0, 8),)),
        "query_weight": heavy_noise(seeds[1], (D, HEADS * HD), D ** -0.5, 0.125, ((0, 8), (1, 4)), (0, 1, 8, 2.0)),
        "key_weight": heavy_noise(seeds[2], (D, HEADS * HD), D ** -0.5, 0.125, ((0, 8), (1, 4)), (0, 1, 8, 2.0)),
        "value_weight": normal_values(seeds[3], (D, HEADS * HD), D ** -0.5, 0.078125, ((0, 8), (1, 4))),
        "output_weight": normal_values(seeds[4], (HEADS * HD, D), (HEADS * HD // 16) ** -0.5, 0.5, ((0, 8), (1, 4))),
        "query_gain": draw_query_gain(jax.random.fold_in(seeds[10], 71), 0),
        "key_gain": draw_key_gain(jax.random.fold_in(seeds[10], 71), 0),
        "frame_index": draw_frame_index(jax.random.fold_in(seeds[10], 71), 0),
        "row_index": draw_row_index(jax.random.fold_in(seeds[10], 71), 0),
        "column_index": draw_column_index(jax.random.fold_in(seeds[10], 71), 0),
    }


NORM_EPS = 0.5

def freq_table(count):
    ratios = jnp.arange(count, dtype=jnp.float32) / count
    return jnp.float32(10000.0) ** (-ratios)

def rope_angles(frame_index, row_index, column_index, head_dim):
    side_pairs = head_dim // 6
    frame_pairs = head_dim // 2 - 2 * side_pairs
    frame_part = frame_index.astype(jnp.float32)[:, None] * freq_table(frame_pairs)[None, :]
    row_part = row_index.astype(jnp.float32)[:, None] * freq_table(side_pairs)[None, :]
    column_part = column_index.astype(jnp.float32)[:, None] * freq_table(side_pairs)[None, :]
    frames, rows, columns = (frame_part.shape[0], row_part.shape[0], column_part.shape[0])
    return jnp.concatenate([jnp.broadcast_to(frame_part[:, None, None, :], (frames, rows, columns, frame_pairs)), jnp.broadcast_to(row_part[None, :, None, :], (frames, rows, columns, side_pairs)), jnp.broadcast_to(column_part[None, None, :, :], (frames, rows, columns, side_pairs))], axis=-1)

def pair_turn(head_dim):
    source = jnp.arange(head_dim)[:, None]
    target = jnp.arange(head_dim)[None, :]
    plus = ((target % 2 == 1) & (source == target - 1)).astype(jnp.float32)
    minus = ((target % 2 == 0) & (source == target + 1)).astype(jnp.float32)
    return plus - minus

def rotate(features, angle, heads_here, head_dim):
    frames, rows, columns = (angle.shape[0], angle.shape[1], angle.shape[2])
    cosine = jnp.repeat(jnp.cos(angle), 2, axis=-1)[:, :, :, None, :]
    sine = jnp.repeat(jnp.sin(angle), 2, axis=-1)[:, :, :, None, :]
    shaped = features.reshape(frames, rows, columns, heads_here, head_dim)
    turned = jnp.dot(shaped.reshape(-1, head_dim), pair_turn(head_dim), precision=lax.Precision.HIGHEST).reshape(shaped.shape)
    rotated = shaped * cosine + turned * sine
    return rotated.astype(jnp.bfloat16).reshape(frames, rows, columns, heads_here * head_dim)

def soft_weights(scores):
    top = lax.optimization_barrier(jnp.max(scores, axis=-1, keepdims=True))
    raised = jnp.exp(scores - top)
    return (raised / lax.optimization_barrier(jnp.sum(raised, axis=-1, keepdims=True))).astype(jnp.bfloat16)

def window_attend(queries, keys, values, first_row, first_column, total_rows, total_columns, heads_here, head_dim):
    frames, rows, columns, width = queries.shape
    across = rows // WT
    along = columns // WT
    area = WT * WT
    scale = 1.0 / math.sqrt(head_dim)

    def tiles(array, extra):
        shaped = array.reshape(frames, across + extra, WT, along + extra, WT, heads_here, head_dim)
        return shaped.transpose(0, 1, 3, 2, 4, 5, 6).reshape(frames, across + extra, along + extra, area, heads_here, head_dim)
    query_tiles = tiles(queries, 0)
    key_tiles = tiles(keys, 2)
    value_tiles = tiles(values, 2)
    offsets = [(down, right) for down in range(3) for right in range(3)]
    key_window = jnp.concatenate([key_tiles[:, down:down + across, right:right + along] for down, right in offsets], axis=3)
    value_window = jnp.concatenate([value_tiles[:, down:down + across, right:right + along] for down, right in offsets], axis=3)
    tile_rows = first_row + jnp.arange(across)
    tile_columns = first_column + jnp.arange(along)
    inside = []
    for down, right in offsets:
        row_ok = (tile_rows + down - 1 >= 0) & (tile_rows + down - 1 < total_rows)
        column_ok = (tile_columns + right - 1 >= 0) & (tile_columns + right - 1 < total_columns)
        inside.append(row_ok[:, None] & column_ok[None, :])
    allowed = jnp.repeat(jnp.stack(inside, axis=-1), area, axis=-1)
    scores = jnp.einsum('fabqhd,fabkhd->fabhqk', query_tiles.astype(jnp.float32), key_window.astype(jnp.float32)) * scale
    scores = jnp.where(allowed[None, :, :, None, None, :], scores, -jnp.inf)
    weights = soft_weights(scores)
    mixed = jnp.einsum('fabhqk,fabkhd->fabqhd', weights.astype(jnp.float32), value_window.astype(jnp.float32)).astype(jnp.bfloat16)
    mixed = mixed.reshape(frames, across, along, WT, WT, heads_here, head_dim)
    return mixed.transpose(0, 1, 3, 2, 4, 5, 6).reshape(frames, rows, columns, width)

def frame_attend(queries, keys, values, heads_here, head_dim):
    frames = queries.shape[0]
    scale = 1.0 / math.sqrt(head_dim)
    query_rows = queries.reshape(frames, -1, heads_here, head_dim).astype(jnp.float32)
    key_rows = keys.reshape(frames, -1, heads_here, head_dim).astype(jnp.float32)
    value_rows = values.reshape(frames, -1, heads_here, head_dim).astype(jnp.float32)
    scores = jnp.einsum('fphd,gphd->phfg', query_rows, key_rows) * scale
    weights = soft_weights(scores)
    mixed = jnp.einsum('phfg,gphd->fphd', weights.astype(jnp.float32), value_rows).astype(jnp.bfloat16)
    return mixed.reshape(queries.shape)

def to_grid(tokens, frames, side):
    width = tokens.shape[-1]
    shaped = tokens.reshape(DEV_ROWS, GRID_W, frames, side, side, width)
    return shaped.transpose(2, 0, 3, 1, 4, 5).reshape(frames, DEV_ROWS * side, GRID_W * side, width)

def from_grid(grid, side):
    frames, width = (grid.shape[0], grid.shape[-1])
    shaped = grid.reshape(frames, DEV_ROWS, side, GRID_W, side, width)
    return shaped.transpose(1, 3, 0, 2, 4, 5).reshape(-1, width)

def reference(latents, query_weight, key_weight, value_weight, output_weight, query_gain, key_gain, frame_index, row_index, column_index):
    frames, side, width = (latents.shape[1], latents.shape[2], latents.shape[4])
    full_width = query_weight.shape[1]
    heads_all = full_width // HD
    tokens = latents.reshape(-1, width)
    query_lin = jnp.dot(tokens, query_weight, preferred_element_type=jnp.float32)
    key_lin = jnp.dot(tokens, key_weight, preferred_element_type=jnp.float32)
    values = jnp.dot(tokens, value_weight, preferred_element_type=jnp.float32).astype(jnp.bfloat16)
    query_norm = query_lin * lax.rsqrt(lax.optimization_barrier(jnp.sum(query_lin * query_lin, axis=1)) / full_width + NORM_EPS)[:, None] * query_gain
    key_norm = key_lin * lax.rsqrt(lax.optimization_barrier(jnp.sum(key_lin * key_lin, axis=1)) / full_width + NORM_EPS)[:, None] * key_gain
    angle = rope_angles(frame_index, row_index, column_index, HD)
    queries = rotate(to_grid(query_norm, frames, side), angle, heads_all, HD)
    keys = rotate(to_grid(key_norm, frames, side), angle, heads_all, HD)
    values_grid = to_grid(values, frames, side)
    margin = ((0, 0), (WT, WT), (WT, WT), (0, 0))
    keys_padded = jnp.pad(keys, margin)
    values_padded = jnp.pad(values_grid, margin)
    tile_rows = queries.shape[1] // WT
    tile_columns = queries.shape[2] // WT

    def one_frame(items):
        query_frame, key_frame, value_frame = items
        return window_attend(query_frame[None], key_frame[None], value_frame[None], 0, 0, tile_rows, tile_columns, heads_all, HD)[0]
    spatial = lax.map(one_frame, (queries, keys_padded, values_padded))
    mixed = frame_attend(queries, keys, spatial, heads_all, HD)
    result = jnp.dot(from_grid(mixed, side), output_weight, preferred_element_type=jnp.float32).astype(jnp.bfloat16)
    return result.reshape(latents.shape)
```

```python
import functools
import math

import jax
import jax.numpy as jnp
import numpy as np
from jax import lax
from jax.experimental import pallas as pl
from jax.experimental.pallas import tpu as pltpu
from jax.sharding import PartitionSpec as P

HEADS = 20
HD = 128
WT = 4
DEV_ROWS = 4


NORM_EPS = 0.5


def lane_tables(head_dim):
    side_pairs = head_dim // 6
    frame_pairs = head_dim // 2 - 2 * side_pairs

    def lanes(before, count, after):
        table = np.power(10000.0, -np.arange(count) / count)
        return np.repeat(np.pad(table, (before, after)), 2)

    tables = np.zeros((8, head_dim), np.float32)
    tables[0] = lanes(0, frame_pairs, 2 * side_pairs)
    tables[1] = lanes(frame_pairs, side_pairs, side_pairs)
    tables[2] = lanes(frame_pairs + side_pairs, side_pairs, 0)
    return tables


CUBE = 8


class Cube:
    def __init__(self, stride):
        me = lax.axis_index("hw")
        within = lax.rem(me, stride) if stride > 1 else 0
        place = lax.div(me, stride) if stride > 1 else me
        core = lax.rem(place, 2)
        x = lax.rem(lax.div(place, 2), 2)
        y = lax.div(place, 4)
        self.place = place
        self.other = [place + 1 - 2 * core, place + 2 - 4 * x, place + 4 - 8 * y]
        self.diagonal = place + 2 - 4 * x + 4 - 8 * y
        self.devices = [{"hw": other * stride + within} for other in self.other]
        self.chip = lax.div(place, 2)
        self.chips = [
            self.chip,
            self.chip + 1 - 2 * x,
            self.chip + 2 - 4 * y,
            self.chip + 3 - 2 * x - 4 * y,
        ]

    def barrier(self, line):
        semaphore = pltpu.get_barrier_semaphore()
        for peers in line:
            peers.greet(semaphore)
        for device in self.devices:
            pl.semaphore_signal(semaphore, inc=1, device_id=device, device_id_type=pl.DeviceIdType.MESH)
        count = sum((peers.number() for peers in line), len(self.devices))
        pl.semaphore_wait(semaphore, count)


class Exchange:
    def __init__(self, cube, held, send, receive, rows, lanes=None):
        core_place, x_place, y_place = cube.other
        half = rows * SPLIT // 10 // 16 * 16

        def part(place, low, size):
            start = pl.multiple_of(lax.rem(place, 2) * rows + low, 16)
            if lanes is None:
                return held.at[lax.div(place, 2), pl.ds(start, size)]
            return held.at[lax.div(place, 2), pl.ds(start, size), lanes]

        def copy(at, place, low, size, partner):
            ref = part(place, low, size)
            return pltpu.make_async_remote_copy(
                src_ref=ref,
                dst_ref=ref,
                send_sem=send.at[at],
                recv_sem=receive.at[at],
                device_id=cube.devices[partner],
                device_id_type=pl.DeviceIdType.MESH,
            )

        rest = rows - half
        self.own = part(cube.place, 0, rows)
        moves = [
            (cube.place, 0, rows, 1),
            (cube.place, 0, rows, 2),
            (cube.place, 0, rows, 0),
            (x_place, 0, rows, 0),
            (y_place, 0, rows, 0),
            (x_place, 0, half, 2),
            (y_place, half, rest, 1),
            (cube.diagonal, 0, half, 0),
            (cube.diagonal, half, rest, 0),
        ]
        self.copy = lambda at: copy(at, *moves[at])

    def start(self, *which):
        for at in which:
            self.copy(at).start()

    def begin(self):
        self.start(0, 1, 2)

    def arrived(self, *which):
        for at in which:
            self.copy(at).wait_recv()

    def near(self):
        self.arrived(0)
        self.start(5, 3)
        self.arrived(1)
        self.start(6, 4)

    def far(self):
        self.arrived(5)
        self.start(7)
        self.arrived(6)
        self.start(8)

    def sent(self):
        for at in range(9):
            self.copy(at).wait_send()


class Peers:
    def __init__(self, parts, send, receive):
        self.count = lax.axis_size("head")
        self.me = lax.axis_index("head")
        self.parts, self.send, self.receive = parts, send, receive

    def device(self, step):
        return {"head": lax.rem(self.me + step, self.count)}

    def greet(self, semaphore):
        for step in range(1, self.count):
            pl.semaphore_signal(
                semaphore,
                inc=1,
                device_id=self.device(step),
                device_id_type=pl.DeviceIdType.MESH,
            )

    def number(self):
        return self.count - 1

    def copy(self, at, step, group):
        ref = self.parts.at[group, at]
        return pltpu.make_async_remote_copy(
            src_ref=ref,
            dst_ref=ref,
            send_sem=self.send.at[at, step - 1],
            recv_sem=self.receive.at[at, step - 1],
            device_id=self.device(step),
            device_id_type=pl.DeviceIdType.MESH,
        )

    def start(self, at):
        for step in range(1, self.count):
            self.copy(at, step, self.me).start()

    def finish(self, at):
        for step in range(1, self.count):
            self.copy(at, step, lax.rem(self.me + self.count - step, self.count)).wait_recv()

    def sent(self, at):
        for step in range(1, self.count):
            self.copy(at, step, self.me).wait_send()


class Line:
    def __init__(self, blocks, send, receive):
        self.count = lax.axis_size("head")
        self.me = lax.axis_index("head")
        self.blocks, self.send, self.receive = blocks, send, receive

    def neighbour(self, side):
        return self.me + 1 if side == 0 else self.me - 1

    def has(self, side):
        return self.me < self.count - 1 if side == 0 else self.me > 0

    def origin(self, side, far):
        return self.me - far if side == 0 else self.me + far

    def holds(self, side, far):
        return self.me >= far if side == 0 else self.me + far < self.count

    def copy(self, side, far, at, group):
        ref = self.blocks(group, at)
        return pltpu.make_async_remote_copy(
            src_ref=ref,
            dst_ref=ref,
            send_sem=self.send.at[side, far, at],
            recv_sem=self.receive.at[side, far, at],
            device_id={"head": self.neighbour(side)},
            device_id_type=pl.DeviceIdType.MESH,
        )

    def start(self, side, far, at):
        @pl.when(self.has(side) & self.holds(side, far))
        def _():
            self.copy(side, far, at, self.origin(side, far)).start()

    def relay(self, far, at):
        for side in range(2):
            @pl.when(self.holds(side, far + 1))
            def _():
                self.copy(side, far, at, self.origin(side, far + 1)).wait_recv()

            if far + 2 < self.count:
                self.start(side, far + 1, at)

    def sent(self, parts):
        for side in range(2):
            for far in range(self.count - 1):
                @pl.when(self.has(side) & self.holds(side, far))
                def _():
                    @pl.loop(0, parts)
                    def _(at):
                        self.copy(side, far, at, self.origin(side, far)).wait_send()


def ones(me, count):
    return 1 - lax.div(me + 1, count) + lax.div(me + count - 1, count)


class Grid:
    def __init__(self, grid_columns, side):
        place = lax.axis_index("hw")
        self.row, self.column = lax.div(place, grid_columns), lax.rem(place, grid_columns)
        self.place, self.columns = place, grid_columns
        self.edge, self.body = WT * side, side * side
        self.slots = min(3, grid_columns)
        self.own = self.column if grid_columns == 2 else self.slots // 2
        self.parts = [
            pl.ds(self.edge, self.body),
            pl.ds(0, self.edge),
            pl.ds(self.edge + self.body, self.edge),
        ]

    def first_column(self):
        return 0 if self.columns == 2 else self.column - self.slots // 2

    def has(self, way):
        return [
            self.row > 0,
            self.row < DEV_ROWS - 1,
            self.column > 0,
            self.column < self.columns - 1,
        ][way]

    def device(self, way):
        step = [-self.columns, self.columns, -1, 1][way]
        return {"hw": self.place + step}

    def greet(self, semaphore):
        for way in range(4):
            @pl.when(self.has(way))
            def _():
                pl.semaphore_signal(
                    semaphore,
                    inc=1,
                    device_id=self.device(way),
                    device_id_type=pl.DeviceIdType.MESH,
                )

    def number(self):
        return ones(self.row, DEV_ROWS) + ones(self.column, self.columns)

    def clear(self, pad):
        for way in range(2):
            @pl.when(jnp.logical_not(self.has(way)))
            def _():
                for slot in range(self.slots):
                    place = pad.at[slot, :, self.parts[1 + way], :]
                    place[...] = jnp.zeros(place.shape, pad.dtype)

        if self.columns > 2:
            for way in (2, 3):
                @pl.when(jnp.logical_not(self.has(way)))
                def _():
                    place = pad.at[0 if way == 2 else self.slots - 1]
                    place[...] = jnp.zeros(place.shape, pad.dtype)


class Halo:
    def __init__(self, grid, pad, lanes, sems):
        self.grid, self.pad, self.lanes = grid, pad, lanes
        self.send, self.receive, self.side_send, self.side_receive = sems

    def at(self, slot, pixels):
        return self.pad.at[slot, :, pixels, self.lanes]

    def vertical(self, way):
        grid = self.grid
        low = grid.edge if way == 0 else grid.body
        return pltpu.make_async_remote_copy(
            src_ref=self.at(grid.own, pl.ds(low, grid.edge)),
            dst_ref=self.at(grid.own, grid.parts[2 - way]),
            send_sem=self.send.at[way],
            recv_sem=self.receive.at[way],
            device_id=grid.device(way),
            device_id_type=pl.DeviceIdType.MESH,
        )

    def sideways(self, way, part):
        grid = self.grid
        if grid.columns == 2:
            slot = grid.own
        else:
            slot = grid.slots - 1 if way == 2 else 0
        return pltpu.make_async_remote_copy(
            src_ref=self.at(grid.own, grid.parts[part]),
            dst_ref=self.at(slot, grid.parts[part]),
            send_sem=self.side_send.at[way - 2, part],
            recv_sem=self.side_receive.at[way - 2, part],
            device_id=grid.device(way),
            device_id_type=pl.DeviceIdType.MESH,
        )

    def start(self):
        for way in range(2):
            @pl.when(self.grid.has(way))
            def _():
                self.vertical(way).start()
        for way in (2, 3):
            @pl.when(self.grid.has(way))
            def _():
                self.sideways(way, 0).start()

    def relay(self):
        for came in range(2):
            @pl.when(self.grid.has(came))
            def _():
                self.vertical(1 - came).wait_recv()
                for way in (2, 3):
                    @pl.when(self.grid.has(way))
                    def _():
                        self.sideways(way, 1 + came).start()

    def finish(self):
        for came in (2, 3):
            @pl.when(self.grid.has(came))
            def _():
                self.sideways(5 - came, 0).wait_recv()
                for part in range(2):
                    @pl.when(self.grid.has(part))
                    def _():
                        self.sideways(5 - came, 1 + part).wait_recv()

    def sent(self):
        for way in range(2):
            @pl.when(self.grid.has(way))
            def _():
                self.vertical(way).wait_send()
        for way in (2, 3):
            @pl.when(self.grid.has(way))
            def _():
                self.sideways(way, 0).wait_send()
                for part in range(2):
                    @pl.when(self.grid.has(part))
                    def _():
                        self.sideways(way, 1 + part).wait_send()


def weigh(scores, allowed):
    scores = jnp.where(allowed, scores, -jnp.inf)
    raised = jnp.exp(scores - jnp.max(scores, axis=-1, keepdims=True))
    return (raised * (1.0 / jnp.sum(raised, axis=-1, keepdims=True))).astype(jnp.bfloat16)


def score(queries, keys):
    return lax.dot_general(
        queries, keys, (((1,), (1,)), ((), ())), preferred_element_type=jnp.float32
    ) * (1.0 / math.sqrt(HD))


SPLIT = 6
STRIP = 16
KEY, QUERY = 0, 1


def block_kernel(
    stride, grid_columns, frames, side,
    tokens_hbm, query_hbm, key_hbm, value_hbm, output_hbm,
    query_gain, key_gain, lanes_ref, frame_index, row_index, column_index,
    result_ref,
    tokens, held, held_value, held_output, sums, trig, query_ref, key_pad, value_pad,
    temporal, spatial, picked, mixed, parts,
    local, send, receive, value_send, value_receive, output_send, output_receive,
    parts_send, parts_receive, line_send, line_receive,
    halo_send, halo_receive, side_send, side_receive,
):
    cube = Cube(stride)
    rows, group_width = query_hbm.shape
    depth = 2 * rows
    output_rows, columns = output_hbm.shape
    heads_here = group_width // HD
    slab = columns // heads_here
    count = tokens.shape[0]
    area = side * side
    block = count // 2

    def head_of(at):
        return pl.ds(pl.multiple_of(at * HD, HD), HD)

    weights = [Exchange(cube, held.at[at], send.at[at], receive.at[at], rows) for at in range(2)]

    def value(at):
        return Exchange(
            cube, held_value, value_send.at[at], value_receive.at[at], rows, head_of(at)
        )

    def slab_of(at):
        return pl.ds(pl.multiple_of(at * slab, 128), slab)

    def output(at):
        return Exchange(
            cube, held_output, output_send.at[at], output_receive.at[at], output_rows, slab_of(at)
        )

    mine = lax.rem(cube.place, 2)
    loads = [
        pltpu.make_async_copy(key_hbm, weights[KEY].own, local.at[0]),
        pltpu.make_async_copy(query_hbm, weights[QUERY].own, local.at[1]),
        pltpu.make_async_copy(tokens_hbm, tokens, local.at[2]),
        pltpu.make_async_copy(
            value_hbm,
            held_value.at[cube.chip, pl.ds(pl.multiple_of(mine * rows, 16), rows)],
            local.at[3],
        ),
        pltpu.make_async_copy(
            output_hbm,
            held_output.at[cube.chip, pl.ds(pl.multiple_of(mine * output_rows, 16), output_rows)],
            local.at[4],
        ),
    ]
    for load in loads:
        load.start()

    peers = Peers(parts, parts_send, parts_receive)
    line = Line(lambda group, at: mixed.at[group, :, :, head_of(at)], line_send, line_receive)
    grid = Grid(grid_columns, side)

    def halo(pad, lanes, at):
        return Halo(
            grid, pad, lanes,
            (halo_send.at[at], halo_receive.at[at], side_send.at[at], side_receive.at[at]),
        )

    key_halo = halo(key_pad, pl.ds(0, group_width), heads_here)

    def value_halo(at):
        return halo(value_pad, head_of(at), at)

    cube.barrier((peers, grid))
    key, query = weights[KEY], weights[QUERY]
    loads[0].wait()
    key.begin()
    loads[1].wait()
    query.begin()

    grid.clear(key_pad)
    grid.clear(value_pad)
    pixel = lax.broadcasted_iota(jnp.int32, (side, HD), 0)
    across = jnp.zeros((side, HD), jnp.float32)
    for at in range(side):
        here = column_index[grid.column * side + at].astype(jnp.float32)
        across = jnp.where(pixel == at, here, across)
    across = across * lanes_ref[2:3, :]

    @pl.loop(0, frames)
    def _(frame):
        along = frame_index[frame].astype(jnp.float32) * lanes_ref[0:1, :]
        for at in range(side):
            down = row_index[grid.row * side + at].astype(jnp.float32) * lanes_ref[1:2, :]
            angle = along + down + across
            here = pl.ds(pl.multiple_of(frame * area + at * side, 8), side)
            trig[0, here, :] = jnp.cos(angle)
            trig[1, here, :] = jnp.sin(angle)

    def multiply(at, lane):
        chip = cube.chips[lane]

        @pl.loop(0, 2)
        def _(step):
            here = pl.ds(pl.multiple_of(step * block, block), block)
            product = jnp.dot(
                tokens[here, pl.ds(pl.multiple_of(chip * depth, 128), depth)],
                held[at, chip],
                preferred_element_type=jnp.float32,
            )
            if lane == 0:
                sums[at, here, :] = product
            else:
                sums[at, here, :] += product

    def near_multiply(at):
        weights[at].arrived(3)
        multiply(at, 1)
        weights[at].arrived(4)
        multiply(at, 2)

    def far_multiply(at):
        weights[at].arrived(7, 8)
        multiply(at, 3)

    def squares(at):
        lin = sums[at]
        parts[peers.me, at] = lax.dot_general(
            jnp.ones((8, group_width), jnp.float32),
            lin * lin,
            (((1,), (1,)), ((), ())),
            precision=lax.Precision.HIGHEST,
            preferred_element_type=jnp.float32,
        )
        peers.start(at)

    span = HD // area
    even = lax.broadcasted_iota(jnp.int32, (HD, HD), 1) % 2 == 0

    def rotate(at, gain, store):
        peers.finish(at)

        @pl.loop(0, count // HD)
        def _(step):
            here = pl.ds(pl.multiple_of(step * HD, HD), HD)
            total = sum(parts[group, at, :, here] for group in range(peers.count))
            scale = lax.rsqrt(total / (HEADS * HD) + NORM_EPS)
            scale = jnp.broadcast_to(scale[0:1, :], (HD, HD)).T
            cosine, sine = trig[0, here, :], trig[1, here, :]
            for head in range(heads_here):
                lanes = slice(head * HD, (head + 1) * HD)
                one = sums[at, here, lanes] * scale * gain[0:1, lanes]
                turned = jnp.where(even, -jnp.roll(one, -1, axis=1), jnp.roll(one, 1, axis=1))
                turned = (one * cosine + turned * sine).astype(jnp.bfloat16)
                store(pl.ds(step * span, span), lanes, turned.reshape(span, area, HD))

    def store_key(where, lanes, block_values):
        key_pad[grid.own, where, grid.parts[0], lanes] = block_values

    def store_query(where, lanes, block_values):
        query_ref[where, :, lanes] = block_values

    loads[2].wait()
    key.arrived(2)
    multiply(KEY, 0)
    query.arrived(2)
    multiply(QUERY, 0)
    key.near()
    near_multiply(KEY)
    loads[3].wait()
    loads[4].wait()
    query.near()
    value(0).begin()
    near_multiply(QUERY)
    key.far()
    far_multiply(KEY)
    squares(KEY)
    rotate(KEY, key_gain, store_key)
    key_halo.start()
    value(1).begin()
    query.far()
    far_multiply(QUERY)
    squares(QUERY)
    value(0).near()
    key_halo.relay()
    rotate(QUERY, query_gain, store_query)

    same = (
        lax.broadcasted_iota(jnp.int32, (frames * STRIP, frames * STRIP), 0) % STRIP
        == lax.broadcasted_iota(jnp.int32, (frames * STRIP, frames * STRIP), 1) % STRIP
    )

    @pl.loop(0, heads_here)
    def _(at):
        head = head_of(at)
        for low in range(0, area, STRIP):
            scores = score(
                query_ref[:, pl.ds(low, STRIP), head].reshape(frames * STRIP, HD),
                key_pad[grid.own, :, pl.ds(grid.edge + low, STRIP), head].reshape(frames * STRIP, HD),
            )
            temporal[at, low // STRIP] = weigh(scores, same)

    tall = side + 2 * WT
    window = tall * side
    keys_here = grid.slots * window
    tiles = side // WT
    query_at = lax.broadcasted_iota(jnp.int32, (area, keys_here), 0)
    key_at = lax.broadcasted_iota(jnp.int32, (area, keys_here), 1)
    key_row = grid.row * tiles - 1 + key_at % window // side // WT
    key_column = (grid.first_column() + key_at // window) * tiles + key_at % side // WT
    down = key_row - grid.row * tiles - query_at // side // WT
    right = key_column - grid.column * tiles - query_at % side // WT
    close = (down >= -1) & (down <= 1) & (right >= -1) & (right <= 1)
    close &= (key_row >= 0) & (key_row < DEV_ROWS * tiles)
    close &= (key_column >= 0) & (key_column < grid_columns * tiles)

    def window_of(pad, frame, head):
        return jnp.concatenate([pad[slot, frame, :, head] for slot in range(grid.slots)], axis=0)

    key_halo.finish()

    @pl.loop(0, heads_here)
    def _(at):
        head = head_of(at)
        for frame in range(frames):
            scores = score(query_ref[frame, :, head], window_of(key_pad, frame, head))
            spatial[at, frame] = weigh(scores, close)

    def begin(at):
        @pl.when(at < heads_here)
        def _():
            value(at).begin()

        @pl.when((at >= heads_here) & (at < 2 * heads_here))
        def _():
            output(at - heads_here).begin()

    def near(at):
        @pl.when(at < heads_here)
        def _():
            value(at).near()

        @pl.when((at >= heads_here) & (at < 2 * heads_here))
        def _():
            output(at - heads_here).near()

    def relays(at):
        for far in range(line.count - 1):
            from_head = at - 1 - far

            @pl.when((from_head >= 0) & (from_head < heads_here))
            def _():
                line.relay(far, from_head)

    half_frames = frames // 2

    @pl.loop(0, heads_here)
    def _(at):
        head = head_of(at)
        weight = value(at)
        weight.far()
        begin(at + 2)
        weight.arrived(2, 3, 4, 7, 8)

        @pl.loop(0, 2)
        def _(step):
            here = pl.ds(pl.multiple_of(step * block, block), block)
            product = sum(
                jnp.dot(
                    tokens[here, chip * depth : (chip + 1) * depth],
                    held_value[chip, :, head],
                    preferred_element_type=jnp.float32,
                )
                for chip in range(CUBE // 2)
            )
            value_pad[grid.own, pl.ds(step * half_frames, half_frames), grid.parts[0], head] = (
                product.astype(jnp.bfloat16).reshape(half_frames, area, HD)
            )

        border = value_halo(at)
        border.start()
        near(at + 1)
        relays(at)
        border.relay()
        border.finish()
        for frame in range(frames):
            picked[frame] = jnp.dot(
                spatial[at, frame],
                window_of(value_pad, frame, head),
                preferred_element_type=jnp.float32,
            ).astype(jnp.bfloat16)
        for low in range(0, area, STRIP):
            mixed[line.me, :, pl.ds(low, STRIP), head] = (
                jnp.dot(
                    temporal[at, low // STRIP],
                    picked[:, pl.ds(low, STRIP), :].reshape(frames * STRIP, HD),
                    preferred_element_type=jnp.float32,
                )
                .astype(jnp.bfloat16)
                .reshape(frames, STRIP, HD)
            )
        line.start(0, 0, at)
        line.start(1, 0, at)

    def project(at):
        @pl.loop(0, 2)
        def _(step):
            total = sum(
                jnp.dot(
                    mixed[group, pl.ds(step * half_frames, half_frames)].reshape(block, group_width),
                    held_output[group, :, slab_of(at)],
                    preferred_element_type=jnp.float32,
                )
                for group in range(line.count)
            )
            here = pl.ds(pl.multiple_of(step * block, block), block)
            result_ref[here, slab_of(at)] = total.astype(result_ref.dtype)

    whole_at = line.count - 2

    @pl.loop(0, heads_here)
    def _(at):
        weight = output(at)
        weight.far()
        begin(heads_here + at + 2)
        near(heads_here + at + 1)
        relays(heads_here + at)
        weight.arrived(2, 3, 4, 7, 8)

        @pl.when(at == whole_at)
        def _():
            @pl.loop(0, whole_at + 1)
            def _(one):
                project(one)

        @pl.when(at > whole_at)
        def _():
            project(at)

    for weight in weights:
        weight.sent()
    for at in range(2):
        peers.sent(at)
    key_halo.sent()

    @pl.loop(0, heads_here)
    def _(at):
        value(at).sent()
        output(at).sent()
        value_halo(at).sent()

    line.sent(heads_here)


def attention_block(
    tokens, query_weight, key_weight, value_weight, output_weight,
    query_gain, key_gain, frame_index, row_index, column_index, stride, grid_columns, frames, side,
):
    count = tokens.shape[0]
    rows, width = query_weight.shape
    output_rows, columns = output_weight.shape
    groups = lax.axis_size("head")
    heads_here = width // HD
    slots = min(3, grid_columns)
    area = side * side
    tall = side * (side + 2 * WT)
    anywhere = pl.BlockSpec(memory_space=pl.ANY)
    vmem = pl.BlockSpec(memory_space=pltpu.VMEM)
    smem = pl.BlockSpec(memory_space=pltpu.SMEM)
    pad = pltpu.VMEM((slots, frames, tall, width), jnp.bfloat16)
    dma = pltpu.SemaphoreType.DMA
    strip = frames * STRIP
    return pl.pallas_call(
        functools.partial(block_kernel, stride, grid_columns, frames, side),
        out_shape=jax.ShapeDtypeStruct((count, columns), jnp.bfloat16),
        in_specs=[anywhere] * 5 + [vmem] * 3 + [smem] * 3,
        out_specs=vmem,
        scratch_shapes=[
            pltpu.VMEM(tokens.shape, tokens.dtype),
            pltpu.VMEM((2, CUBE // 2, 2 * rows, width), query_weight.dtype),
            pltpu.VMEM((CUBE // 2, 2 * rows, width), value_weight.dtype),
            pltpu.VMEM((CUBE // 2, 2 * output_rows, columns), output_weight.dtype),
            pltpu.VMEM((2, count, width), jnp.float32),
            pltpu.VMEM((2, count, HD), jnp.float32),
            pltpu.VMEM((frames, area, width), jnp.bfloat16),
            pad,
            pad,
            pltpu.VMEM((heads_here, area // STRIP, strip, strip), jnp.bfloat16),
            pltpu.VMEM((heads_here, frames, area, slots * tall), jnp.bfloat16),
            pltpu.VMEM((frames, area, HD), jnp.bfloat16),
            pltpu.VMEM((groups, frames, area, width), jnp.bfloat16),
            pltpu.VMEM((groups, 2, 8, count), jnp.float32),
            dma((5,)),
            dma((2, 9)),
            dma((2, 9)),
            dma((heads_here, 9)),
            dma((heads_here, 9)),
            dma((heads_here, 9)),
            dma((heads_here, 9)),
            dma((2, groups - 1)),
            dma((2, groups - 1)),
            dma((2, groups - 1, heads_here)),
            dma((2, groups - 1, heads_here)),
            dma((heads_here + 1, 2)),
            dma((heads_here + 1, 2)),
            dma((heads_here + 1, 2, 3)),
            dma((heads_here + 1, 2, 3)),
        ],
        compiler_params=pltpu.CompilerParams(
            collective_id=0, has_side_effects=True, vmem_limit_bytes=60 * 1024 * 1024
        ),
        name="attention_block",
    )(
        tokens, query_weight, key_weight, value_weight, output_weight,
        query_gain[None], key_gain[None], jnp.asarray(lane_tables(HD)),
        frame_index, row_index, column_index,
    )


def pregather(weight, stride):
    if stride == 1:
        return weight
    count = lax.axis_size("hw")
    groups = [list(range(first, first + stride)) for first in range(0, count, stride)]
    return lax.all_gather(weight, "hw", axis=0, tiled=True, axis_index_groups=groups)


def per_device(
    latents,
    query_weight,
    key_weight,
    value_weight,
    output_weight,
    query_gain,
    key_gain,
    frame_index,
    row_index,
    column_index,
):
    frames, side, width = (latents.shape[1], latents.shape[2], latents.shape[4])
    tokens = latents.reshape(frames * side * side, width)
    grid_columns = lax.axis_size("hw") // DEV_ROWS
    stride = lax.axis_size("hw") // CUBE
    result = attention_block(
        tokens,
        *(pregather(w, stride) for w in (query_weight, key_weight, value_weight, output_weight)),
        query_gain, key_gain, frame_index, row_index, column_index,
        stride, grid_columns, frames, side,
    )
    return result.reshape(1, frames, side, side, output_weight.shape[1])


def solution(mesh):
    placed = (
        P("hw", None, None, None, None),
        P("hw", "head"),
        P("hw", "head"),
        P("hw", "head"),
        P("hw", "head"),
        P("head"),
        P("head"),
        P(),
        P(),
        P(),
    )
    return jax.shard_map(
        per_device,
        mesh=mesh,
        in_specs=placed,
        out_specs=P("hw", None, None, None, "head"),
        check_vma=False,
    )
```

```python
import functools
import math

import jax
import jax.numpy as jnp
import numpy as np
from jax import lax
from jax.experimental import pallas as pl
from jax.experimental.pallas import tpu as pltpu
from jax.sharding import PartitionSpec as P

HEADS = 20
HD = 128
WT = 4
DEV_ROWS = 4


NORM_EPS = 0.5


def lane_tables(head_dim):
    side_pairs = head_dim // 6
    frame_pairs = head_dim // 2 - 2 * side_pairs

    def lanes(before, count, after):
        table = np.power(10000.0, -np.arange(count) / count)
        return np.repeat(np.pad(table, (before, after)), 2)

    tables = np.zeros((8, head_dim), np.float32)
    tables[0] = lanes(0, frame_pairs, 2 * side_pairs)
    tables[1] = lanes(frame_pairs, side_pairs, side_pairs)
    tables[2] = lanes(frame_pairs + side_pairs, side_pairs, 0)
    return tables


CUBE = 8


class Cube:
    def __init__(self, stride):
        me = lax.axis_index("hw")
        within = lax.rem(me, stride) if stride > 1 else 0
        place = lax.div(me, stride) if stride > 1 else me
        core = lax.rem(place, 2)
        x = lax.rem(lax.div(place, 2), 2)
        y = lax.div(place, 4)
        self.place = place
        self.other = [place + 1 - 2 * core, place + 2 - 4 * x, place + 4 - 8 * y]
        self.diagonal = place + 2 - 4 * x + 4 - 8 * y
        self.devices = [{"hw": other * stride + within} for other in self.other]
        self.chip = lax.div(place, 2)
        self.chips = [
            self.chip,
            self.chip + 1 - 2 * x,
            self.chip + 2 - 4 * y,
            self.chip + 3 - 2 * x - 4 * y,
        ]

    def barrier(self, line):
        semaphore = pltpu.get_barrier_semaphore()
        for peers in line:
            peers.greet(semaphore)
        for device in self.devices:
            pl.semaphore_signal(semaphore, inc=1, device_id=device, device_id_type=pl.DeviceIdType.MESH)
        count = sum((peers.number() for peers in line), len(self.devices))
        pl.semaphore_wait(semaphore, count)


class Exchange:
    def __init__(self, cube, held, send, receive, rows, tenths, lanes=None):
        core_place, x_place, y_place = cube.other
        half = rows * tenths // 10 // 16 * 16

        def part(place, low, size):
            start = pl.multiple_of(lax.rem(place, 2) * rows + low, 16)
            if lanes is None:
                return held.at[lax.div(place, 2), pl.ds(start, size)]
            return held.at[lax.div(place, 2), pl.ds(start, size), lanes]

        def copy(at, place, low, size, partner):
            ref = part(place, low, size)
            return pltpu.make_async_remote_copy(
                src_ref=ref,
                dst_ref=ref,
                send_sem=send.at[at],
                recv_sem=receive.at[at],
                device_id=cube.devices[partner],
                device_id_type=pl.DeviceIdType.MESH,
            )

        rest = rows - half
        self.own = part(cube.place, 0, rows)
        moves = [
            (cube.place, 0, rows, 1),
            (cube.place, 0, rows, 2),
            (cube.place, 0, rows, 0),
            (x_place, 0, rows, 0),
            (y_place, 0, rows, 0),
            (x_place, 0, half, 2),
            (y_place, half, rest, 1),
            (cube.diagonal, 0, half, 0),
            (cube.diagonal, half, rest, 0),
        ]
        self.copy = lambda at: copy(at, *moves[at])

    def start(self, *which):
        for at in which:
            self.copy(at).start()

    def begin(self):
        self.start(0, 1, 2)

    def arrived(self, *which):
        for at in which:
            self.copy(at).wait_recv()

    def near(self):
        self.arrived(0)
        self.start(5, 3)
        self.arrived(1)
        self.start(6, 4)

    def far(self):
        self.arrived(5)
        self.start(7)
        self.arrived(6)
        self.start(8)

    def sent(self):
        for at in range(9):
            self.copy(at).wait_send()


class Peers:
    def __init__(self, parts, send, receive):
        self.count = lax.axis_size("head")
        self.me = lax.axis_index("head")
        self.parts, self.send, self.receive = parts, send, receive

    def device(self, step):
        return {"head": lax.rem(self.me + step, self.count)}

    def greet(self, semaphore):
        for step in range(1, self.count):
            pl.semaphore_signal(
                semaphore,
                inc=1,
                device_id=self.device(step),
                device_id_type=pl.DeviceIdType.MESH,
            )

    def number(self):
        return self.count - 1

    def copy(self, at, step, group):
        ref = self.parts.at[group, at]
        return pltpu.make_async_remote_copy(
            src_ref=ref,
            dst_ref=ref,
            send_sem=self.send.at[at, step - 1],
            recv_sem=self.receive.at[at, step - 1],
            device_id=self.device(step),
            device_id_type=pl.DeviceIdType.MESH,
        )

    def start(self, at):
        for step in range(1, self.count):
            self.copy(at, step, self.me).start()

    def finish(self, at):
        for step in range(1, self.count):
            self.copy(at, step, lax.rem(self.me + self.count - step, self.count)).wait_recv()

    def sent(self, at):
        for step in range(1, self.count):
            self.copy(at, step, self.me).wait_send()


class Line:
    def __init__(self, blocks, send, receive):
        self.count = lax.axis_size("head")
        self.me = lax.axis_index("head")
        self.blocks, self.send, self.receive = blocks, send, receive

    def neighbour(self, side):
        return self.me + 1 if side == 0 else self.me - 1

    def has(self, side):
        return self.me < self.count - 1 if side == 0 else self.me > 0

    def origin(self, side, far):
        return self.me - far if side == 0 else self.me + far

    def holds(self, side, far):
        return self.me >= far if side == 0 else self.me + far < self.count

    def copy(self, side, far, at, group):
        ref = self.blocks(group, at)
        return pltpu.make_async_remote_copy(
            src_ref=ref,
            dst_ref=ref,
            send_sem=self.send.at[side, far, at],
            recv_sem=self.receive.at[side, far, at],
            device_id={"head": self.neighbour(side)},
            device_id_type=pl.DeviceIdType.MESH,
        )

    def start(self, side, far, at):
        @pl.when(self.has(side) & self.holds(side, far))
        def _():
            self.copy(side, far, at, self.origin(side, far)).start()

    def relay(self, far, at):
        for side in range(2):
            @pl.when(self.holds(side, far + 1))
            def _():
                self.copy(side, far, at, self.origin(side, far + 1)).wait_recv()

            if far + 2 < self.count:
                self.start(side, far + 1, at)

    def sent(self, parts):
        for side in range(2):
            for far in range(self.count - 1):
                @pl.when(self.has(side) & self.holds(side, far))
                def _():
                    @pl.loop(0, parts)
                    def _(at):
                        self.copy(side, far, at, self.origin(side, far)).wait_send()


def ones(me, count):
    return 1 - lax.div(me + 1, count) + lax.div(me + count - 1, count)


class Grid:
    def __init__(self, grid_columns, side):
        place = lax.axis_index("hw")
        self.row, self.column = lax.div(place, grid_columns), lax.rem(place, grid_columns)
        self.place, self.columns = place, grid_columns
        self.edge, self.body = WT * side, side * side
        self.slots = min(3, grid_columns)
        self.own = self.column if grid_columns == 2 else self.slots // 2
        self.parts = [
            pl.ds(self.edge, self.body),
            pl.ds(0, self.edge),
            pl.ds(self.edge + self.body, self.edge),
        ]

    def first_column(self):
        return 0 if self.columns == 2 else self.column - self.slots // 2

    def has(self, way):
        return [
            self.row > 0,
            self.row < DEV_ROWS - 1,
            self.column > 0,
            self.column < self.columns - 1,
        ][way]

    def device(self, way):
        step = [-self.columns, self.columns, -1, 1][way]
        return {"hw": self.place + step}

    def greet(self, semaphore):
        for way in range(4):
            @pl.when(self.has(way))
            def _():
                pl.semaphore_signal(
                    semaphore,
                    inc=1,
                    device_id=self.device(way),
                    device_id_type=pl.DeviceIdType.MESH,
                )

    def number(self):
        return ones(self.row, DEV_ROWS) + ones(self.column, self.columns)

    def clear(self, pad):
        for way in range(2):
            @pl.when(jnp.logical_not(self.has(way)))
            def _():
                for slot in range(self.slots):
                    place = pad.at[slot, :, self.parts[1 + way], :]
                    place[...] = jnp.zeros(place.shape, pad.dtype)

        if self.columns > 2:
            for way in (2, 3):
                @pl.when(jnp.logical_not(self.has(way)))
                def _():
                    place = pad.at[0 if way == 2 else self.slots - 1]
                    place[...] = jnp.zeros(place.shape, pad.dtype)


class Halo:
    def __init__(self, grid, pad, lanes, sems):
        self.grid, self.pad, self.lanes = grid, pad, lanes
        self.send, self.receive, self.side_send, self.side_receive = sems

    def at(self, slot, pixels):
        return self.pad.at[slot, :, pixels, self.lanes]

    def vertical(self, way):
        grid = self.grid
        low = grid.edge if way == 0 else grid.body
        return pltpu.make_async_remote_copy(
            src_ref=self.at(grid.own, pl.ds(low, grid.edge)),
            dst_ref=self.at(grid.own, grid.parts[2 - way]),
            send_sem=self.send.at[way],
            recv_sem=self.receive.at[way],
            device_id=grid.device(way),
            device_id_type=pl.DeviceIdType.MESH,
        )

    def sideways(self, way, part):
        grid = self.grid
        if grid.columns == 2:
            slot = grid.own
        else:
            slot = grid.slots - 1 if way == 2 else 0
        return pltpu.make_async_remote_copy(
            src_ref=self.at(grid.own, grid.parts[part]),
            dst_ref=self.at(slot, grid.parts[part]),
            send_sem=self.side_send.at[way - 2, part],
            recv_sem=self.side_receive.at[way - 2, part],
            device_id=grid.device(way),
            device_id_type=pl.DeviceIdType.MESH,
        )

    def start(self):
        self.start_vertical()
        self.start_sideways()

    def start_vertical(self):
        for way in range(2):
            @pl.when(self.grid.has(way))
            def _():
                self.vertical(way).start()

    def start_sideways(self):
        for way in (2, 3):
            @pl.when(self.grid.has(way))
            def _():
                self.sideways(way, 0).start()

    def relay(self):
        for came in range(2):
            @pl.when(self.grid.has(came))
            def _():
                self.vertical(1 - came).wait_recv()
                for way in (2, 3):
                    @pl.when(self.grid.has(way))
                    def _():
                        self.sideways(way, 1 + came).start()

    def finish(self):
        for came in (2, 3):
            @pl.when(self.grid.has(came))
            def _():
                self.sideways(5 - came, 0).wait_recv()
                for part in range(2):
                    @pl.when(self.grid.has(part))
                    def _():
                        self.sideways(5 - came, 1 + part).wait_recv()

    def sent(self):
        for way in range(2):
            @pl.when(self.grid.has(way))
            def _():
                self.vertical(way).wait_send()
        for way in (2, 3):
            @pl.when(self.grid.has(way))
            def _():
                self.sideways(way, 0).wait_send()
                for part in range(2):
                    @pl.when(self.grid.has(part))
                    def _():
                        self.sideways(way, 1 + part).wait_send()


def weigh(scores, allowed):
    scores = jnp.where(allowed, scores, -jnp.inf)
    raised = jnp.exp(scores - jnp.max(scores, axis=-1, keepdims=True))
    return (raised * (1.0 / jnp.sum(raised, axis=-1, keepdims=True))).astype(jnp.bfloat16)


def score(queries, keys):
    return lax.dot_general(
        queries, keys, (((1,), (1,)), ((), ())), preferred_element_type=jnp.float32
    ) * (1.0 / math.sqrt(HD))


SPLIT = 7
DEPTH = 3
STRIP = 16
KEY, QUERY = 0, 1


def block_kernel(
    stride, grid_columns, frames, side,
    tokens_hbm, query_hbm, key_hbm, value_hbm, output_hbm,
    query_gain, key_gain, lanes_ref, frame_index, row_index, column_index,
    result_hbm,
    result_ref, tokens, held, held_value, held_output, sums, trig, query_ref, key_pad, value_pad,
    temporal, spatial, picked, mixed, parts,
    local, store, send, receive, value_send, value_receive, output_send, output_receive,
    parts_send, parts_receive, line_send, line_receive,
    halo_send, halo_receive, side_send, side_receive,
):
    cube = Cube(stride)
    rows, group_width = query_hbm.shape
    depth = 2 * rows
    output_rows, columns = output_hbm.shape
    heads_here = group_width // HD
    slab = columns // heads_here
    count = tokens.shape[0]
    area = side * side
    block = count // 2

    def head_of(at):
        return pl.ds(pl.multiple_of(at * HD, HD), HD)

    weights = [Exchange(cube, held.at[at], send.at[at], receive.at[at], rows, 5) for at in range(2)]

    def value(at):
        return Exchange(
            cube, held_value, value_send.at[at], value_receive.at[at], rows, SPLIT, head_of(at)
        )

    def slab_of(at):
        return pl.ds(pl.multiple_of(at * slab, 128), slab)

    def output(at):
        return Exchange(
            cube, held_output, output_send.at[at], output_receive.at[at], output_rows, SPLIT, slab_of(at)
        )

    mine = lax.rem(cube.place, 2)
    loads = [
        pltpu.make_async_copy(key_hbm, weights[KEY].own, local.at[0]),
        pltpu.make_async_copy(query_hbm, weights[QUERY].own, local.at[1]),
        pltpu.make_async_copy(tokens_hbm, tokens, local.at[2]),
        pltpu.make_async_copy(
            value_hbm,
            held_value.at[cube.chip, pl.ds(pl.multiple_of(mine * rows, 16), rows)],
            local.at[3],
        ),
        pltpu.make_async_copy(
            output_hbm,
            held_output.at[cube.chip, pl.ds(pl.multiple_of(mine * output_rows, 16), output_rows)],
            local.at[4],
        ),
    ]
    for at in (3, 0, 1, 2, 4):
        loads[at].start()

    peers = Peers(parts, parts_send, parts_receive)
    line = Line(lambda group, at: mixed.at[group, :, :, head_of(at)], line_send, line_receive)
    grid = Grid(grid_columns, side)

    def halo(pad, lanes, at):
        return Halo(
            grid, pad, lanes,
            (halo_send.at[at], halo_receive.at[at], side_send.at[at], side_receive.at[at]),
        )

    key_halo = halo(key_pad, pl.ds(0, group_width), heads_here)

    def value_halo(at):
        return halo(value_pad, head_of(at), at)

    with jax.named_scope("barrier"):
        cube.barrier((peers, grid))
    key, query = weights[KEY], weights[QUERY]
    loads[3].wait()
    value(0).begin()
    loads[0].wait()
    key.begin()
    loads[1].wait()
    query.begin()

    with jax.named_scope("clear"):
        grid.clear(key_pad)
        grid.clear(value_pad)
    pixel = lax.broadcasted_iota(jnp.int32, (side, HD), 0)
    across = jnp.zeros((side, HD), jnp.float32)
    for at in range(side):
        here = column_index[grid.column * side + at].astype(jnp.float32)
        across = jnp.where(pixel == at, here, across)
    across = across * lanes_ref[2:3, :]

    @pl.loop(0, frames)
    @jax.named_scope("trig")
    def _(frame):
        along = frame_index[frame].astype(jnp.float32) * lanes_ref[0:1, :]
        for at in range(side):
            down = row_index[grid.row * side + at].astype(jnp.float32) * lanes_ref[1:2, :]
            angle = along + down + across
            here = pl.ds(pl.multiple_of(frame * area + at * side, 8), side)
            trig[0, here, :] = jnp.cos(angle)
            trig[1, here, :] = jnp.sin(angle)

    def multiply(at, lane):
        chip = cube.chips[lane]

        @pl.loop(0, 2)
        def _(step):
            here = pl.ds(pl.multiple_of(step * block, block), block)
            product = jnp.dot(
                tokens[here, pl.ds(pl.multiple_of(chip * depth, 128), depth)],
                held[at, chip],
                preferred_element_type=jnp.float32,
            )
            if lane == 0:
                sums[at, here, :] = product
            else:
                sums[at, here, :] += product

    def near_multiply(at):
        weights[at].arrived(3)
        multiply(at, 1)
        weights[at].arrived(4)
        multiply(at, 2)

    def far_multiply(at):
        weights[at].arrived(7, 8)
        multiply(at, 3)

    def squares(at):
        lin = sums[at]
        parts[peers.me, at] = lax.dot_general(
            jnp.ones((8, group_width), jnp.float32),
            lin * lin,
            (((1,), (1,)), ((), ())),
            precision=lax.Precision.HIGHEST,
            preferred_element_type=jnp.float32,
        )
        peers.start(at)

    span = HD // area
    even = lax.broadcasted_iota(jnp.int32, (HD, HD), 1) % 2 == 0

    def rotate(at, gain, store):
        @pl.loop(0, count // HD)
        def _(step):
            here = pl.ds(pl.multiple_of(step * HD, HD), HD)
            total = sum(parts[group, at, :, here] for group in range(peers.count))
            scale = lax.rsqrt(total / (HEADS * HD) + NORM_EPS)
            scale = jnp.broadcast_to(scale[0:1, :], (HD, HD)).T
            cosine, sine = trig[0, here, :], trig[1, here, :]
            for head in range(heads_here):
                lanes = slice(head * HD, (head + 1) * HD)
                one = sums[at, here, lanes] * scale * gain[lanes].reshape(1, HD)
                turned = jnp.where(even, -jnp.roll(one, -1, axis=1), jnp.roll(one, 1, axis=1))
                turned = (one * cosine + turned * sine).astype(jnp.bfloat16)
                store(pl.ds(step * span, span), lanes, turned.reshape(span, area, HD))

    def store_key(where, lanes, block_values):
        key_pad[grid.own, where, grid.parts[0], lanes] = block_values

    def store_query(where, lanes, block_values):
        query_ref[where, :, lanes] = block_values

    same = (
        lax.broadcasted_iota(jnp.int32, (frames * STRIP, frames * STRIP), 0) % STRIP
        == lax.broadcasted_iota(jnp.int32, (frames * STRIP, frames * STRIP), 1) % STRIP
    )

    tall = side + 2 * WT
    window = tall * side
    keys_here = grid.slots * window
    tiles = side // WT
    query_at = lax.broadcasted_iota(jnp.int32, (area, keys_here), 0)
    key_at = lax.broadcasted_iota(jnp.int32, (area, keys_here), 1)
    key_row = grid.row * tiles - 1 + key_at % window // side // WT
    key_column = (grid.first_column() + key_at // window) * tiles + key_at % side // WT
    down = key_row - grid.row * tiles - query_at // side // WT
    right = key_column - grid.column * tiles - query_at % side // WT
    close = (down >= -1) & (down <= 1) & (right >= -1) & (right <= 1)
    close &= (key_row >= 0) & (key_row < DEV_ROWS * tiles)
    close &= (key_column >= 0) & (key_column < grid_columns * tiles)

    def window_of(pad, frame, head):
        return jnp.concatenate([pad[slot, frame, :, head] for slot in range(grid.slots)], axis=0)

    mark = jax.named_scope
    half_frames = frames // 2

    def multiply_value(at):
        head = head_of(at)
        with mark("v_arrived"):
            value(at).arrived(2, 3, 4, 7, 8)

        @pl.loop(0, 2)
        @jax.named_scope("v_multiply")
        def _(step):
            here = pl.ds(pl.multiple_of(step * block, block), block)
            product = sum(
                jnp.dot(
                    tokens[here, chip * depth : (chip + 1) * depth],
                    held_value[chip, :, head],
                    preferred_element_type=jnp.float32,
                )
                for chip in range(CUBE // 2)
            )
            value_pad[grid.own, pl.ds(step * half_frames, half_frames), grid.parts[0], head] = (
                product.astype(jnp.bfloat16).reshape(half_frames, area, HD)
            )

        value_halo(at).start()

    with mark("tokens_wait"):
        loads[2].wait()
    with mark("k0_wait"):
        key.arrived(2)
    with mark("k0"):
        multiply(KEY, 0)
    with mark("q0_wait"):
        query.arrived(2)
    with mark("q0"):
        multiply(QUERY, 0)
    with mark("v_near0"):
        value(0).near()
    with mark("k_near"):
        key.near()
    with mark("k12"):
        near_multiply(KEY)
    loads[4].wait()
    with mark("q_near"):
        query.near()
    with mark("q12"):
        near_multiply(QUERY)
    with mark("v_far"):
        value(0).far()
    multiply_value(0)
    value(1).begin()
    with mark("k_far"):
        key.far()
    with mark("k3"):
        far_multiply(KEY)
    with mark("k_squares"):
        squares(KEY)
    with mark("k_peers"):
        peers.finish(KEY)
    with mark("k_rotate"):
        rotate(KEY, key_gain, store_key)
    key_halo.start_vertical()
    with mark("q_far"):
        query.far()
    key_halo.start_sideways()
    with mark("q3"):
        far_multiply(QUERY)
    with mark("q_squares"):
        squares(QUERY)
    with mark("v_halo0"):
        value_halo(0).relay()
    with mark("v_near1"):
        value(1).near()
    value(2).begin()
    with mark("q_peers"):
        peers.finish(QUERY)
    with mark("q_rotate"):
        rotate(QUERY, query_gain, store_query)
    with mark("k_halo_relay"):
        key_halo.relay()

    @jax.named_scope("weights")
    def make_weights(at):
        head = head_of(at)
        for low in range(0, area, STRIP):
            scores = score(
                query_ref[:, pl.ds(low, STRIP), head].reshape(frames * STRIP, HD),
                key_pad[grid.own, :, pl.ds(grid.edge + low, STRIP), head].reshape(frames * STRIP, HD),
            )
            temporal[low // STRIP] = weigh(scores, same)
        for frame in range(frames):
            scores = score(query_ref[frame, :, head], window_of(key_pad, frame, head))
            spatial[frame] = weigh(scores, close)

    @jax.named_scope("attend")
    def attend(at):
        head = head_of(at)
        for frame in range(frames):
            picked[frame] = jnp.dot(
                spatial[frame],
                window_of(value_pad, frame, head),
                preferred_element_type=jnp.float32,
            ).astype(jnp.bfloat16)
        for low in range(0, area, STRIP):
            mixed[line.me, :, pl.ds(low, STRIP), head] = (
                jnp.dot(
                    temporal[low // STRIP],
                    picked[:, pl.ds(low, STRIP), :].reshape(frames * STRIP, HD),
                    preferred_element_type=jnp.float32,
                )
                .astype(jnp.bfloat16)
                .reshape(frames, STRIP, HD)
            )

    def relays(at):
        for far in range(line.count - 1):
            from_head = at - 2 - far

            @pl.when((from_head >= 1) & (from_head < heads_here))
            def _():
                line.relay(far, from_head)

    def share(at):
        with mark("v_halo_finish"):
            value_halo(at).finish()
        attend(at)
        line.start(0, 0, at)
        line.start(1, 0, at)

    with mark("k_halo_finish"):
        key_halo.finish()
    make_weights(0)
    share(0)
    with mark("early_sent"):
        for weight in weights:
            weight.sent()
        for at in range(2):
            peers.sent(at)
        key_halo.sent()
    value(3).begin()
    with mark("line0"):
        line.relay(0, 0)

    @pl.loop(1, heads_here + 1)
    def _(at):
        @pl.when(at < heads_here - 1)
        @jax.named_scope("v_near")
        def _():
            value(at + 1).near()

        @pl.when(at >= heads_here - 1)
        @jax.named_scope("v_near")
        def _():
            output(at + 1 - heads_here).near()

        @pl.when(at < heads_here)
        @jax.named_scope("v_far")
        def _():
            value(at).far()

        @pl.when(at == heads_here)
        @jax.named_scope("v_far")
        def _():
            output(0).far()

        @pl.when(at > 1)
        def _():
            make_weights(at - 1)
            with mark("v_halo_relay"):
                value_halo(at - 1).relay()

        @pl.when(at < heads_here)
        def _():
            multiply_value(at)

        @pl.when(at < heads_here - DEPTH)
        def _():
            value(at + DEPTH).begin()

        @pl.when((at >= heads_here - DEPTH) & (at < heads_here - 1))
        def _():
            output(at + DEPTH - heads_here).begin()

        @pl.when(at == heads_here - 1)
        def _():
            @pl.loop(DEPTH - 1, heads_here)
            def _(one):
                output(one).begin()

        @pl.when(at > 1)
        def _():
            share(at - 1)

        for far in range(1, line.count - 1):
            @pl.when(at == far)
            @jax.named_scope("line0")
            def _():
                line.relay(far, 0)

        with mark("v_line_relays"):
            relays(at)


    def stored(at):
        return pltpu.make_async_copy(
            result_ref.at[:, slab_of(at)], result_hbm.at[:, slab_of(at)], store.at[at]
        )

    def project(at):
        @pl.loop(0, 2)
        @jax.named_scope("project")
        def _(step):
            total = sum(
                jnp.dot(
                    mixed[group, pl.ds(step * half_frames, half_frames)].reshape(block, group_width),
                    held_output[group, :, slab_of(at)],
                    preferred_element_type=jnp.float32,
                )
                for group in range(line.count)
            )
            here = pl.ds(pl.multiple_of(step * block, block), block)
            result_ref[here, slab_of(at)] = total.astype(result_ref.dtype)

        stored(at).start()

    whole_at = 2

    @pl.loop(0, heads_here)
    def _(at):
        @pl.when(at < heads_here - 2)
        @jax.named_scope("o_near")
        def _():
            output(at + 2).near()

        @pl.when(at < heads_here - 1)
        @jax.named_scope("o_far")
        def _():
            output(at + 1).far()

        @pl.when(at <= whole_at)
        @jax.named_scope("o_line_relays")
        def _():
            relays(heads_here + 1 + at)

        with mark("v_sent"):
            value(at).sent()
            value_halo(at).sent()
        with mark("o_arrived"):
            output(at).arrived(2, 3, 4, 7, 8)

        @pl.when(at == whole_at)
        def _():
            @pl.loop(0, whole_at + 1)
            def _(one):
                project(one)

        @pl.when(at > whole_at)
        def _():
            project(at)

    with mark("sent"):
        @pl.loop(0, heads_here)
        def _(at):
            output(at).sent()

        line.sent(heads_here)

        @pl.loop(0, heads_here)
        def _(at):
            stored(at).wait()


def attention_block(
    tokens, query_weight, key_weight, value_weight, output_weight,
    query_gain, key_gain, frame_index, row_index, column_index, stride, grid_columns, frames, side,
):
    count = tokens.shape[0]
    rows, width = query_weight.shape
    output_rows, columns = output_weight.shape
    groups = lax.axis_size("head")
    heads_here = width // HD
    slots = min(3, grid_columns)
    area = side * side
    tall = side * (side + 2 * WT)
    anywhere = pl.BlockSpec(memory_space=pl.ANY)
    vmem = pl.BlockSpec(memory_space=pltpu.VMEM)
    smem = pl.BlockSpec(memory_space=pltpu.SMEM)
    pad = pltpu.VMEM((slots, frames, tall, width), jnp.bfloat16)
    dma = pltpu.SemaphoreType.DMA
    strip = frames * STRIP
    return pl.pallas_call(
        functools.partial(block_kernel, stride, grid_columns, frames, side),
        out_shape=jax.ShapeDtypeStruct((count, columns), jnp.bfloat16),
        in_specs=[anywhere] * 5 + [vmem] * 3 + [smem] * 3,
        out_specs=anywhere,
        scratch_shapes=[
            pltpu.VMEM((count, columns), jnp.bfloat16),
            pltpu.VMEM(tokens.shape, tokens.dtype),
            pltpu.VMEM((2, CUBE // 2, 2 * rows, width), query_weight.dtype),
            pltpu.VMEM((CUBE // 2, 2 * rows, width), value_weight.dtype),
            pltpu.VMEM((CUBE // 2, 2 * output_rows, columns), output_weight.dtype),
            pltpu.VMEM((2, count, width), jnp.float32),
            pltpu.VMEM((2, count, HD), jnp.float32),
            pltpu.VMEM((frames, area, width), jnp.bfloat16),
            pad,
            pad,
            pltpu.VMEM((area // STRIP, strip, strip), jnp.bfloat16),
            pltpu.VMEM((frames, area, slots * tall), jnp.bfloat16),
            pltpu.VMEM((frames, area, HD), jnp.bfloat16),
            pltpu.VMEM((groups, frames, area, width), jnp.bfloat16),
            pltpu.VMEM((groups, 2, 8, count), jnp.float32),
            dma((5,)),
            dma((heads_here,)),
            dma((2, 9)),
            dma((2, 9)),
            dma((heads_here, 9)),
            dma((heads_here, 9)),
            dma((heads_here, 9)),
            dma((heads_here, 9)),
            dma((2, groups - 1)),
            dma((2, groups - 1)),
            dma((2, groups - 1, heads_here)),
            dma((2, groups - 1, heads_here)),
            dma((heads_here + 1, 2)),
            dma((heads_here + 1, 2)),
            dma((heads_here + 1, 2, 3)),
            dma((heads_here + 1, 2, 3)),
        ],
        compiler_params=pltpu.CompilerParams(
            collective_id=0, has_side_effects=True, vmem_limit_bytes=60 * 1024 * 1024
        ),
        name="attention_block",
    )(
        tokens, query_weight, key_weight, value_weight, output_weight,
        query_gain, key_gain, jnp.asarray(lane_tables(HD)),
        frame_index, row_index, column_index,
    )


def pregather(weight, stride):
    if stride == 1:
        return weight
    count = lax.axis_size("hw")
    groups = [list(range(first, first + stride)) for first in range(0, count, stride)]
    return lax.all_gather(weight, "hw", axis=0, tiled=True, axis_index_groups=groups)


def per_device(
    latents,
    query_weight,
    key_weight,
    value_weight,
    output_weight,
    query_gain,
    key_gain,
    frame_index,
    row_index,
    column_index,
):
    frames, side, width = (latents.shape[1], latents.shape[2], latents.shape[4])
    tokens = latents.reshape(frames * side * side, width)
    grid_columns = lax.axis_size("hw") // DEV_ROWS
    stride = lax.axis_size("hw") // CUBE
    result = attention_block(
        tokens,
        *(pregather(w, stride) for w in (query_weight, key_weight, value_weight, output_weight)),
        query_gain, key_gain, frame_index, row_index, column_index,
        stride, grid_columns, frames, side,
    )
    return result.reshape(1, frames, side, side, output_weight.shape[1])


def solution(mesh):
    placed = (
        P("hw", None, None, None, None),
        P("hw", "head"),
        P("hw", "head"),
        P("hw", "head"),
        P("hw", "head"),
        P("head"),
        P("head"),
        P(),
        P(),
        P(),
    )
    return jax.shard_map(
        per_device,
        mesh=mesh,
        in_specs=placed,
        out_specs=P("hw", None, None, None, "head"),
        check_vma=False,
    )
```

```python
import functools
import math

import jax
import jax.numpy as jnp
import numpy as np
from jax import lax
from jax.experimental import pallas as pl
from jax.experimental.pallas import tpu as pltpu
from jax.sharding import PartitionSpec as P

HEADS = 20
HD = 128
WT = 4
DEV_ROWS = 4


NORM_EPS = 0.5


def lane_tables(head_dim):
    side_pairs = head_dim // 6
    frame_pairs = head_dim // 2 - 2 * side_pairs

    def lanes(before, count, after):
        table = np.power(10000.0, -np.arange(count) / count)
        return np.repeat(np.pad(table, (before, after)), 2)

    tables = np.zeros((8, head_dim), np.float32)
    tables[0] = lanes(0, frame_pairs, 2 * side_pairs)
    tables[1] = lanes(frame_pairs, side_pairs, side_pairs)
    tables[2] = lanes(frame_pairs + side_pairs, side_pairs, 0)
    return tables


CUBE = 8


class Cube:
    def __init__(self, stride):
        me = lax.axis_index("hw")
        within = lax.rem(me, stride) if stride > 1 else 0
        place = lax.div(me, stride) if stride > 1 else me
        core = lax.rem(place, 2)
        x = lax.rem(lax.div(place, 2), 2)
        y = lax.div(place, 4)
        self.place = place
        self.other = [place + 1 - 2 * core, place + 2 - 4 * x, place + 4 - 8 * y]
        self.diagonal = place + 2 - 4 * x + 4 - 8 * y
        self.devices = [{"hw": other * stride + within} for other in self.other]
        self.chip = lax.div(place, 2)
        self.chips = [
            self.chip,
            self.chip + 1 - 2 * x,
            self.chip + 2 - 4 * y,
            self.chip + 3 - 2 * x - 4 * y,
        ]

    def barrier(self, line):
        semaphore = pltpu.get_barrier_semaphore()
        for peers in line:
            peers.greet(semaphore)
        for device in self.devices:
            pl.semaphore_signal(semaphore, inc=1, device_id=device, device_id_type=pl.DeviceIdType.MESH)
        count = sum((peers.number() for peers in line), len(self.devices))
        pl.semaphore_wait(semaphore, count)


class Exchange:
    def __init__(self, cube, held, send, receive, rows, tenths, lanes=None):
        arrivals = [0, 1, 2, 3, 4, 5, 6, 7, 8] if lanes is None else [0, 1, 2, 2, 2, 3, 4, 2, 2]
        core_place, x_place, y_place = cube.other
        half = rows * tenths // 10 // 16 * 16

        def part(place, low, size):
            start = pl.multiple_of(lax.rem(place, 2) * rows + low, 16)
            if lanes is None:
                return held.at[lax.div(place, 2), pl.ds(start, size)]
            return held.at[lax.div(place, 2), pl.ds(start, size), lanes]

        def copy(at, place, low, size, partner):
            ref = part(place, low, size)
            return pltpu.make_async_remote_copy(
                src_ref=ref,
                dst_ref=ref,
                send_sem=send.at[0 if partner else 1],
                recv_sem=receive.at[arrivals[at]],
                device_id=cube.devices[partner],
                device_id_type=pl.DeviceIdType.MESH,
            )

        rest = rows - half
        self.own = part(cube.place, 0, rows)
        moves = [
            (cube.place, 0, rows, 1),
            (cube.place, 0, rows, 2),
            (cube.place, 0, rows, 0),
            (x_place, 0, rows, 0),
            (y_place, 0, rows, 0),
            (x_place, 0, half, 2),
            (y_place, half, rest, 1),
            (cube.diagonal, 0, half, 0),
            (cube.diagonal, half, rest, 0),
        ]
        self.copy = lambda at: copy(at, *moves[at])

        def together(chips, size, sent_by, arrived_at):
            ref = held.at[pl.ds(0, chips), pl.ds(0, size)]
            if lanes is not None:
                ref = held.at[pl.ds(0, chips), pl.ds(0, size), lanes]
            return pltpu.make_async_remote_copy(
                src_ref=ref,
                dst_ref=ref,
                send_sem=send.at[sent_by],
                recv_sem=receive.at[arrived_at],
                device_id=cube.devices[0],
                device_id_type=pl.DeviceIdType.MESH,
            )

        self.links = lambda: together(3, rows, 0, 0)
        self.within = lambda: together(2, 2 * rows, 1, 2)

    def start(self, *which):
        for at in which:
            self.copy(at).start()

    def begin(self):
        self.start(0, 1, 2)

    def arrived(self, *which):
        for at in which:
            self.copy(at).wait_recv()

    def near(self):
        self.arrived(0)
        self.start(5, 3)
        self.arrived(1)
        self.start(6, 4)

    def far(self):
        self.arrived(5)
        self.start(7)
        self.arrived(6)
        self.start(8)

    def arrived_all(self):
        self.within().wait_recv()

    def sent(self):
        self.links().wait_send()
        self.within().wait_send()


class Peers:
    def __init__(self, parts, send, receive):
        self.count = lax.axis_size("head")
        self.me = lax.axis_index("head")
        self.parts, self.send, self.receive = parts, send, receive

    def device(self, step):
        return {"head": lax.rem(self.me + step, self.count)}

    def greet(self, semaphore):
        for step in range(1, self.count):
            pl.semaphore_signal(
                semaphore,
                inc=1,
                device_id=self.device(step),
                device_id_type=pl.DeviceIdType.MESH,
            )

    def number(self):
        return self.count - 1

    def copy(self, at, step, group):
        ref = self.parts.at[group, at]
        return pltpu.make_async_remote_copy(
            src_ref=ref,
            dst_ref=ref,
            send_sem=self.send.at[at, step - 1],
            recv_sem=self.receive.at[at, step - 1],
            device_id=self.device(step),
            device_id_type=pl.DeviceIdType.MESH,
        )

    def start(self, at):
        for step in range(1, self.count):
            self.copy(at, step, self.me).start()

    def finish(self, at):
        for step in range(1, self.count):
            self.copy(at, step, lax.rem(self.me + self.count - step, self.count)).wait_recv()

    def sent(self, at):
        for step in range(1, self.count):
            self.copy(at, step, self.me).wait_send()


class Line:
    def __init__(self, blocks, send, receive):
        self.count = lax.axis_size("head")
        self.me = lax.axis_index("head")
        self.blocks, self.send, self.receive = blocks, send, receive

    def neighbour(self, side):
        return self.me + 1 if side == 0 else self.me - 1

    def has(self, side):
        return self.me < self.count - 1 if side == 0 else self.me > 0

    def origin(self, side, far):
        return self.me - far if side == 0 else self.me + far

    def holds(self, side, far):
        return self.me >= far if side == 0 else self.me + far < self.count

    def copy(self, side, far, at, group):
        ref = self.blocks(group, at)
        return pltpu.make_async_remote_copy(
            src_ref=ref,
            dst_ref=ref,
            send_sem=self.send.at[side, far],
            recv_sem=self.receive.at[side, far, 0 if at is None else at],
            device_id={"head": self.neighbour(side)},
            device_id_type=pl.DeviceIdType.MESH,
        )

    def start(self, side, far, at):
        @pl.when(self.has(side) & self.holds(side, far))
        def _():
            self.copy(side, far, at, self.origin(side, far)).start()

    def relay(self, far, at):
        for side in range(2):
            @pl.when(self.holds(side, far + 1))
            def _():
                self.copy(side, far, at, self.origin(side, far + 1)).wait_recv()

            if far + 2 < self.count:
                self.start(side, far + 1, at)

    def sent(self):
        for side in range(2):
            for far in range(self.count - 1):
                @pl.when(self.has(side) & self.holds(side, far))
                def _():
                    self.copy(side, far, None, self.origin(side, far)).wait_send()


def ones(me, count):
    return 1 - lax.div(me + 1, count) + lax.div(me + count - 1, count)


class Grid:
    def __init__(self, grid_columns, side):
        place = lax.axis_index("hw")
        self.row, self.column = lax.div(place, grid_columns), lax.rem(place, grid_columns)
        self.place, self.columns = place, grid_columns
        self.edge, self.body = WT * side, side * side
        self.slots = min(3, grid_columns)
        self.own = self.column if grid_columns == 2 else self.slots // 2
        self.parts = [
            pl.ds(self.edge, self.body),
            pl.ds(0, self.edge),
            pl.ds(self.edge + self.body, self.edge),
        ]

    def first_column(self):
        return 0 if self.columns == 2 else self.column - self.slots // 2

    def has(self, way):
        return [
            self.row > 0,
            self.row < DEV_ROWS - 1,
            self.column > 0,
            self.column < self.columns - 1,
        ][way]

    def device(self, way):
        step = [-self.columns, self.columns, -1, 1][way]
        return {"hw": self.place + step}

    def greet(self, semaphore):
        for way in range(4):
            @pl.when(self.has(way))
            def _():
                pl.semaphore_signal(
                    semaphore,
                    inc=1,
                    device_id=self.device(way),
                    device_id_type=pl.DeviceIdType.MESH,
                )

    def number(self):
        return ones(self.row, DEV_ROWS) + ones(self.column, self.columns)

    def clear(self, pad):
        for way in range(2):
            @pl.when(jnp.logical_not(self.has(way)))
            def _():
                for slot in range(self.slots):
                    place = pad.at[slot, :, self.parts[1 + way], :]
                    place[...] = jnp.zeros(place.shape, pad.dtype)

        if self.columns > 2:
            for way in (2, 3):
                @pl.when(jnp.logical_not(self.has(way)))
                def _():
                    place = pad.at[0 if way == 2 else self.slots - 1]
                    place[...] = jnp.zeros(place.shape, pad.dtype)


class Halo:
    def __init__(self, grid, pad, lanes, sems, stage=None):
        self.grid, self.pad, self.lanes, self.stage = grid, pad, lanes, stage
        self.send, self.receive, self.side_send, self.side_receive = sems[:4]
        if stage is not None:
            self.half_send, self.half_receive = sems[4:]
        self.frames = pad.shape[1]
        self.direct = pl.ds(0, self.frames if stage is None else self.frames // 2)
        self.rest = pl.ds(self.frames // 2, self.frames // 2)

    def at(self, slot, pixels, frames=None):
        if frames is None:
            frames = pl.ds(0, self.frames)
        return self.pad.at[slot, frames, pixels, self.lanes]

    def border(self, way):
        grid = self.grid
        return pl.ds(grid.edge if way == 0 else grid.body, grid.edge)

    def vertical(self, way):
        grid = self.grid
        return pltpu.make_async_remote_copy(
            src_ref=self.at(grid.own, self.border(way), self.direct),
            dst_ref=self.at(grid.own, grid.parts[2 - way], self.direct),
            send_sem=self.send.at[way],
            recv_sem=self.receive.at[way],
            device_id=grid.device(way),
            device_id_type=pl.DeviceIdType.MESH,
        )

    def second(self, way, move):
        grid = self.grid
        there = self.at(grid.own, grid.parts[2 - way], self.rest)
        step = 1 if way == 1 else -1
        distance = [step, 2 * step, -step][move]
        return pltpu.make_async_remote_copy(
            src_ref=self.stage if move == 2 else self.at(grid.own, self.border(way), self.rest),
            dst_ref=self.stage if move == 1 else there,
            send_sem=self.half_send.at[way, int(move == 2)],
            recv_sem=self.half_receive.at[way, int(move == 1)],
            device_id={"hw": grid.place + distance * grid.columns},
            device_id_type=pl.DeviceIdType.MESH,
        )

    def start_second(self):
        for way in range(2):
            far = self.grid.row == 2 - way

            @pl.when(far)
            def _():
                self.second(way, 1).start()

            @pl.when(self.grid.has(way) & jnp.logical_not(far))
            def _():
                self.second(way, 0).start()

    def forward(self):
        if self.stage is None:
            return
        for way in range(2):
            @pl.when(self.grid.row == (DEV_ROWS - 1) * way)
            def _():
                self.second(way, 1).wait_recv()
                self.second(way, 2).start()

    def sideways(self, way, part):
        grid = self.grid
        if grid.columns == 2:
            slot = grid.own
        else:
            slot = grid.slots - 1 if way == 2 else 0
        return pltpu.make_async_remote_copy(
            src_ref=self.at(grid.own, grid.parts[part]),
            dst_ref=self.at(slot, grid.parts[part]),
            send_sem=self.side_send.at[way - 2, part],
            recv_sem=self.side_receive.at[way - 2, part],
            device_id=grid.device(way),
            device_id_type=pl.DeviceIdType.MESH,
        )

    def start(self):
        self.start_vertical()
        self.start_sideways()

    def start_vertical(self):
        for way in range(2):
            @pl.when(self.grid.has(way))
            def _():
                self.vertical(way).start()
        if self.stage is not None:
            self.start_second()

    def start_sideways(self):
        for way in (2, 3):
            @pl.when(self.grid.has(way))
            def _():
                self.sideways(way, 0).start()

    def relay(self):
        for came in range(2):
            @pl.when(self.grid.has(came))
            def _():
                self.vertical(1 - came).wait_recv()
                if self.stage is not None:
                    self.second(1 - came, 0).wait_recv()
                for way in (2, 3):
                    @pl.when(self.grid.has(way))
                    def _():
                        self.sideways(way, 1 + came).start()

    def finish(self):
        for came in (2, 3):
            @pl.when(self.grid.has(came))
            def _():
                self.sideways(5 - came, 0).wait_recv()
                for part in range(2):
                    @pl.when(self.grid.has(part))
                    def _():
                        self.sideways(5 - came, 1 + part).wait_recv()

    def sent(self):
        for way in range(2):
            @pl.when(self.grid.has(way))
            def _():
                self.vertical(way).wait_send()
                if self.stage is not None:
                    self.second(way, 0).wait_send()

            if self.stage is not None:
                @pl.when(self.grid.row == (DEV_ROWS - 1) * way)
                def _():
                    self.second(way, 2).wait_send()
        for way in (2, 3):
            @pl.when(self.grid.has(way))
            def _():
                self.sideways(way, 0).wait_send()
                for part in range(2):
                    @pl.when(self.grid.has(part))
                    def _():
                        self.sideways(way, 1 + part).wait_send()


def weigh(scores, allowed):
    scores = jnp.where(allowed, scores, -jnp.inf)
    raised = jnp.exp(scores - jnp.max(scores, axis=-1, keepdims=True))
    return (raised * (1.0 / jnp.sum(raised, axis=-1, keepdims=True))).astype(jnp.bfloat16)


def score(queries, keys):
    return lax.dot_general(
        queries, keys, (((1,), (1,)), ((), ())), preferred_element_type=jnp.float32
    ) * (1.0 / math.sqrt(HD))


SPLIT = 7
DEPTH = 3
STRIP = 16
KEY, QUERY = 0, 1


def block_kernel(
    stride, grid_columns, frames, side,
    tokens_hbm, query_hbm, key_hbm, value_hbm, output_hbm,
    query_gain, key_gain, lanes_ref, frame_index, row_index, column_index,
    result_hbm,
    result_ref, total, tokens, held, held_value, held_output, sums, trig, query_ref, key_pad, value_pad,
    temporal, spatial, picked, mixed, parts, stage,
    local, store, send, receive, value_send, value_receive, output_send, output_receive,
    parts_send, parts_receive, line_send, line_receive,
    halo_send, halo_receive, side_send, side_receive, half_send, half_receive,
):
    cube = Cube(stride)
    rows, group_width = query_hbm.shape
    depth = 2 * rows
    output_rows, columns = output_hbm.shape
    heads_here = group_width // HD
    slab = columns // heads_here
    count = tokens.shape[0]
    area = side * side
    block = count // 2

    def head_of(at):
        return pl.ds(pl.multiple_of(at * HD, HD), HD)

    weights = [Exchange(cube, held.at[at], send.at[at], receive.at[at], rows, 5) for at in range(2)]

    def value(at):
        return Exchange(
            cube, held_value, value_send.at[at], value_receive.at[at], rows, SPLIT, head_of(at)
        )

    def slab_of(at):
        return pl.ds(pl.multiple_of(at * slab, 128), slab)

    def output(at):
        return Exchange(
            cube, held_output, output_send.at[at], output_receive.at[at], output_rows, SPLIT, slab_of(at)
        )

    mine = lax.rem(cube.place, 2)
    loads = [
        pltpu.make_async_copy(key_hbm, weights[KEY].own, local.at[0]),
        pltpu.make_async_copy(query_hbm, weights[QUERY].own, local.at[1]),
        pltpu.make_async_copy(tokens_hbm, tokens, local.at[2]),
        pltpu.make_async_copy(
            value_hbm,
            held_value.at[cube.chip, pl.ds(pl.multiple_of(mine * rows, 16), rows)],
            local.at[3],
        ),
        pltpu.make_async_copy(
            output_hbm,
            held_output.at[cube.chip, pl.ds(pl.multiple_of(mine * output_rows, 16), output_rows)],
            local.at[4],
        ),
    ]
    for at in (3, 0, 1, 2, 4):
        loads[at].start()

    peers = Peers(parts, parts_send, parts_receive)
    line = Line(
        lambda group, at: mixed.at[group] if at is None else mixed.at[group, :, :, head_of(at)],
        line_send, line_receive,
    )
    grid = Grid(grid_columns, side)

    def halo(pad, lanes, at):
        return Halo(
            grid, pad, lanes,
            (halo_send.at[at], halo_receive.at[at], side_send.at[at], side_receive.at[at]),
        )

    key_halo = halo(key_pad, pl.ds(0, group_width), heads_here)
    if grid_columns == 2:
        key_halo = Halo(
            grid, key_pad, pl.ds(0, group_width),
            (
                halo_send.at[heads_here], halo_receive.at[heads_here],
                side_send.at[heads_here], side_receive.at[heads_here],
                half_send, half_receive,
            ),
            stage,
        )

    def value_halo(at):
        return halo(value_pad, head_of(at), at)

    with jax.named_scope("barrier"):
        cube.barrier((peers, grid))
    key, query = weights[KEY], weights[QUERY]
    loads[3].wait()
    value(0).begin()
    loads[0].wait()
    key.begin()
    loads[1].wait()
    query.begin()

    with jax.named_scope("clear"):
        grid.clear(key_pad)
        grid.clear(value_pad)
    pixel = lax.broadcasted_iota(jnp.int32, (side, HD), 0)
    across = jnp.zeros((side, HD), jnp.float32)
    for at in range(side):
        here = column_index[grid.column * side + at].astype(jnp.float32)
        across = jnp.where(pixel == at, here, across)
    across = across * lanes_ref[2:3, :]

    @pl.loop(0, frames)
    @jax.named_scope("trig")
    def _(frame):
        along = frame_index[frame].astype(jnp.float32) * lanes_ref[0:1, :]
        for at in range(side):
            down = row_index[grid.row * side + at].astype(jnp.float32) * lanes_ref[1:2, :]
            angle = along + down + across
            here = pl.ds(pl.multiple_of(frame * area + at * side, 8), side)
            trig[0, here, :] = jnp.cos(angle)
            trig[1, here, :] = jnp.sin(angle)

    def multiply(at, lane):
        chip = cube.chips[lane]

        @pl.loop(0, 2)
        def _(step):
            here = pl.ds(pl.multiple_of(step * block, block), block)
            product = jnp.dot(
                tokens[here, pl.ds(pl.multiple_of(chip * depth, 128), depth)],
                held[at, chip],
                preferred_element_type=jnp.float32,
            )
            if lane == 0:
                sums[at, here, :] = product
            else:
                sums[at, here, :] += product

    def near_multiply(at):
        weights[at].arrived(3)
        multiply(at, 1)
        weights[at].arrived(4)
        multiply(at, 2)

    def far_multiply(at):
        weights[at].arrived(7, 8)
        multiply(at, 3)

    def squares(at):
        lin = sums[at]
        parts[peers.me, at] = lax.dot_general(
            jnp.ones((8, group_width), jnp.float32),
            lin * lin,
            (((1,), (1,)), ((), ())),
            precision=lax.Precision.HIGHEST,
            preferred_element_type=jnp.float32,
        )
        peers.start(at)

    span = HD // area
    even = lax.broadcasted_iota(jnp.int32, (HD, HD), 1) % 2 == 0

    def rotate(at, gain, store):
        @pl.loop(0, count // HD)
        def _(step):
            here = pl.ds(pl.multiple_of(step * HD, HD), HD)
            squared = sum(parts[group, at, :, here] for group in range(peers.count))
            scale = lax.rsqrt(squared / (HEADS * HD) + NORM_EPS)
            scale = jnp.broadcast_to(scale[0:1, :], (HD, HD)).T
            cosine, sine = trig[0, here, :], trig[1, here, :]
            for head in range(heads_here):
                lanes = slice(head * HD, (head + 1) * HD)
                one = sums[at, here, lanes] * scale * gain[lanes].reshape(1, HD)
                turned = jnp.where(even, -jnp.roll(one, -1, axis=1), jnp.roll(one, 1, axis=1))
                turned = (one * cosine + turned * sine).astype(jnp.bfloat16)
                store(pl.ds(step * span, span), lanes, turned.reshape(span, area, HD))

    def store_key(where, lanes, block_values):
        key_pad[grid.own, where, grid.parts[0], lanes] = block_values

    def store_query(where, lanes, block_values):
        query_ref[where, :, lanes] = block_values

    same = (
        lax.broadcasted_iota(jnp.int32, (frames * STRIP, frames * STRIP), 0) % STRIP
        == lax.broadcasted_iota(jnp.int32, (frames * STRIP, frames * STRIP), 1) % STRIP
    )

    tall = side + 2 * WT
    window = tall * side
    keys_here = grid.slots * window
    tiles = side // WT
    query_at = lax.broadcasted_iota(jnp.int32, (area, keys_here), 0)
    key_at = lax.broadcasted_iota(jnp.int32, (area, keys_here), 1)
    key_row = grid.row * tiles - 1 + key_at % window // side // WT
    key_column = (grid.first_column() + key_at // window) * tiles + key_at % side // WT
    down = key_row - grid.row * tiles - query_at // side // WT
    right = key_column - grid.column * tiles - query_at % side // WT
    close = (down >= -1) & (down <= 1) & (right >= -1) & (right <= 1)
    close &= (key_row >= 0) & (key_row < DEV_ROWS * tiles)
    close &= (key_column >= 0) & (key_column < grid_columns * tiles)

    def window_of(pad, frame, head):
        return jnp.concatenate([pad[slot, frame, :, head] for slot in range(grid.slots)], axis=0)

    mark = jax.named_scope
    half_frames = frames // 2

    def multiply_value(at):
        head = head_of(at)
        with mark("v_arrived"):
            value(at).arrived_all()

        @pl.loop(0, 2)
        @jax.named_scope("v_multiply")
        def _(step):
            here = pl.ds(pl.multiple_of(step * block, block), block)
            product = sum(
                jnp.dot(
                    tokens[here, chip * depth : (chip + 1) * depth],
                    held_value[chip, :, head],
                    preferred_element_type=jnp.float32,
                )
                for chip in range(CUBE // 2)
            )
            value_pad[grid.own, pl.ds(step * half_frames, half_frames), grid.parts[0], head] = (
                product.astype(jnp.bfloat16).reshape(half_frames, area, HD)
            )

        value_halo(at).start()

    with mark("tokens_wait"):
        loads[2].wait()
    with mark("k0_wait"):
        key.arrived(2)
    with mark("k0"):
        multiply(KEY, 0)
    with mark("q0_wait"):
        query.arrived(2)
    with mark("q0"):
        multiply(QUERY, 0)
    with mark("v_near0"):
        value(0).near()
    with mark("k_near"):
        key.near()
    with mark("k12"):
        near_multiply(KEY)
    loads[4].wait()
    with mark("q_near"):
        query.near()
    with mark("q12"):
        near_multiply(QUERY)
    with mark("v_far"):
        value(0).far()
    multiply_value(0)
    value(1).begin()
    with mark("k_far"):
        key.far()
    with mark("k3"):
        far_multiply(KEY)
    with mark("k_squares"):
        squares(KEY)
    with mark("k_peers"):
        peers.finish(KEY)
    with mark("k_rotate"):
        rotate(KEY, key_gain, store_key)
    key_halo.start_vertical()
    with mark("q_far"):
        query.far()
    key_halo.start_sideways()
    with mark("q3"):
        far_multiply(QUERY)
    with mark("q_squares"):
        squares(QUERY)
    with mark("v_halo0"):
        value_halo(0).relay()
    with mark("v_near1"):
        value(1).near()
    value(2).begin()
    with mark("k_forward"):
        key_halo.forward()
    with mark("q_peers"):
        peers.finish(QUERY)
    with mark("q_rotate"):
        rotate(QUERY, query_gain, store_query)
    with mark("k_halo_relay"):
        key_halo.relay()

    @jax.named_scope("weights")
    def make_weights(at):
        head = head_of(at)
        for low in range(0, area, STRIP):
            scores = score(
                query_ref[:, pl.ds(low, STRIP), head].reshape(frames * STRIP, HD),
                key_pad[grid.own, :, pl.ds(grid.edge + low, STRIP), head].reshape(frames * STRIP, HD),
            )
            temporal[low // STRIP] = weigh(scores, same)
        for frame in range(frames):
            scores = score(query_ref[frame, :, head], window_of(key_pad, frame, head))
            spatial[frame] = weigh(scores, close)

    @jax.named_scope("attend")
    def attend(at):
        head = head_of(at)
        for frame in range(frames):
            picked[frame] = jnp.dot(
                spatial[frame],
                window_of(value_pad, frame, head),
                preferred_element_type=jnp.float32,
            ).astype(jnp.bfloat16)
        for low in range(0, area, STRIP):
            mixed[line.me, :, pl.ds(low, STRIP), head] = (
                jnp.dot(
                    temporal[low // STRIP],
                    picked[:, pl.ds(low, STRIP), :].reshape(frames * STRIP, HD),
                    preferred_element_type=jnp.float32,
                )
                .astype(jnp.bfloat16)
                .reshape(frames, STRIP, HD)
            )

    def relays(at):
        for far in range(line.count - 1):
            from_head = at - 2 - far
            if isinstance(from_head, int) and from_head >= heads_here:
                continue

            @pl.when((from_head >= 2) & (from_head < heads_here))
            def _():
                line.relay(far, from_head)

    def share(at):
        with mark("v_halo_finish"):
            value_halo(at).finish()
        attend(at)
        line.start(0, 0, at)
        line.start(1, 0, at)

    with mark("k_halo_finish"):
        key_halo.finish()
    make_weights(0)
    share(0)
    with mark("early_sent"):
        for weight in weights:
            weight.sent()
        for at in range(2):
            peers.sent(at)
        key_halo.sent()
    with mark("v_far"):
        value(1).far()
    multiply_value(1)
    with mark("v_near"):
        value(2).near()
    value(3).begin()
    value(4).begin()
    make_weights(1)
    with mark("line0"):
        line.relay(0, 0)
    with mark("v_halo_relay"):
        value_halo(1).relay()
    share(1)

    @pl.loop(2, heads_here + 1)
    def _(at):
        @pl.when(at < heads_here - 1)
        @jax.named_scope("v_near")
        def _():
            value(at + 1).near()

        @pl.when(at >= heads_here - 1)
        @jax.named_scope("v_near")
        def _():
            output(at + 1 - heads_here).near()

        @pl.when(at < heads_here)
        @jax.named_scope("v_far")
        def _():
            value(at).far()

        @pl.when(at == heads_here)
        @jax.named_scope("v_far")
        def _():
            output(0).far()

        @pl.when(at > 2)
        def _():
            make_weights(at - 1)
            with mark("v_halo_relay"):
                value_halo(at - 1).relay()

        @pl.when(at < heads_here)
        def _():
            multiply_value(at)

        @pl.when(at < heads_here - DEPTH)
        def _():
            value(at + DEPTH).begin()

        @pl.when(at >= heads_here - DEPTH)
        def _():
            output(at + DEPTH - heads_here).begin()

        @pl.when(at > 2)
        def _():
            share(at - 1)

        for far in range(line.count - 1):
            for first in range(2):
                if first + far > 0:
                    @pl.when(at == far + first + 1)
                    @jax.named_scope("line0")
                    def _():
                        line.relay(far, first)

        with mark("v_line_relays"):
            relays(at)


    def stored(at):
        return pltpu.make_async_copy(
            result_ref.at[:, slab_of(at)], result_hbm.at[:, slab_of(at)], store.at[at]
        )

    def project(at, low, high):
        some = slice(low * HD, high * HD)

        @pl.loop(0, 2)
        @jax.named_scope("project")
        def _(step):
            sum_here = sum(
                jnp.dot(
                    mixed[group, pl.ds(step * half_frames, half_frames), :, some].reshape(
                        block, (high - low) * HD
                    ),
                    held_output[group, some, slab_of(at)],
                    preferred_element_type=jnp.float32,
                )
                for group in range(line.count)
            )
            here = pl.ds(pl.multiple_of(step * block, block), block)
            if low > 0:
                sum_here += total[here, slab_of(at)]
            if high < heads_here:
                total[here, slab_of(at)] = sum_here
            else:
                result_ref[here, slab_of(at)] = sum_here.astype(result_ref.dtype)

        if high == heads_here:
            stored(at).start()

    def project_all(first, last, low, high):
        @pl.loop(first, last)
        def _(at):
            project(at, low, high)

    early = 3
    with mark("o_near"):
        output(2).near()
    output(4).begin()
    with mark("o_line_relays"):
        relays(heads_here + 1)
    with mark("o_far"):
        output(1).far()
    with mark("o_near"):
        output(3).near()
    with mark("o_far"):
        output(0).arrived_all()
        output(1).arrived_all()
    project_all(0, 2, 0, early)
    with mark("o_line_relays"):
        relays(heads_here + 2)
    with mark("o_far"):
        output(2).far()
    with mark("o_near"):
        output(4).near()
    with mark("o_far"):
        output(3).far()
        output(2).arrived_all()
    project_all(2, 3, 0, early)
    with mark("v_sent"):
        @pl.loop(0, heads_here)
        def _(at):
            value(at).sent()
            value_halo(at).sent()

    with mark("o_line_relays"):
        relays(heads_here + 3)
    project_all(0, 3, early, heads_here)
    with mark("o_far"):
        output(4).far()
        output(3).arrived_all()
    project_all(3, 4, 0, heads_here)
    with mark("v_sent"):
        @pl.loop(0, heads_here - 1)
        def _(at):
            output(at).sent()

    with mark("o_far"):
        output(4).arrived_all()
    project_all(4, heads_here, 0, heads_here)
    output(4).sent()

    with mark("sent"):
        line.sent()

        @pl.loop(0, heads_here)
        def _(at):
            stored(at).wait()


def attention_block(
    tokens, query_weight, key_weight, value_weight, output_weight,
    query_gain, key_gain, frame_index, row_index, column_index, stride, grid_columns, frames, side,
):
    count = tokens.shape[0]
    rows, width = query_weight.shape
    output_rows, columns = output_weight.shape
    groups = lax.axis_size("head")
    heads_here = width // HD
    slots = min(3, grid_columns)
    area = side * side
    tall = side * (side + 2 * WT)
    anywhere = pl.BlockSpec(memory_space=pl.ANY)
    vmem = pl.BlockSpec(memory_space=pltpu.VMEM)
    smem = pl.BlockSpec(memory_space=pltpu.SMEM)
    pad = pltpu.VMEM((slots, frames, tall, width), jnp.bfloat16)
    dma = pltpu.SemaphoreType.DMA
    strip = frames * STRIP
    return pl.pallas_call(
        functools.partial(block_kernel, stride, grid_columns, frames, side),
        out_shape=jax.ShapeDtypeStruct((count, columns), jnp.bfloat16),
        in_specs=[anywhere] * 5 + [vmem] * 3 + [smem] * 3,
        out_specs=anywhere,
        scratch_shapes=[
            pltpu.VMEM((count, columns), jnp.bfloat16),
            pltpu.VMEM((count, columns), jnp.float32),
            pltpu.VMEM(tokens.shape, tokens.dtype),
            pltpu.VMEM((2, CUBE // 2, 2 * rows, width), query_weight.dtype),
            pltpu.VMEM((CUBE // 2, 2 * rows, width), value_weight.dtype),
            pltpu.VMEM((CUBE // 2, 2 * output_rows, columns), output_weight.dtype),
            pltpu.VMEM((2, count, width), jnp.float32),
            pltpu.VMEM((2, count, HD), jnp.float32),
            pltpu.VMEM((frames, area, width), jnp.bfloat16),
            pad,
            pad,
            pltpu.VMEM((area // STRIP, strip, strip), jnp.bfloat16),
            pltpu.VMEM((frames, area, slots * tall), jnp.bfloat16),
            pltpu.VMEM((frames, area, HD), jnp.bfloat16),
            pltpu.VMEM((groups, frames, area, width), jnp.bfloat16),
            pltpu.VMEM((groups, 2, 8, count), jnp.float32),
            pltpu.VMEM((frames // 2, WT * side, width), jnp.bfloat16),
            dma((5,)),
            dma((heads_here,)),
            dma((2, 2)),
            dma((2, 9)),
            dma((heads_here, 2)),
            dma((heads_here, 5)),
            dma((heads_here, 2)),
            dma((heads_here, 5)),
            dma((2, groups - 1)),
            dma((2, groups - 1)),
            dma((2, groups - 1)),
            dma((2, groups - 1, heads_here)),
            dma((heads_here + 1, 2)),
            dma((heads_here + 1, 2)),
            dma((heads_here + 1, 2, 3)),
            dma((heads_here + 1, 2, 3)),
            dma((2, 2)),
            dma((2, 2)),
        ],
        compiler_params=pltpu.CompilerParams(
            collective_id=0, has_side_effects=True, vmem_limit_bytes=60 * 1024 * 1024
        ),
        name="attention_block",
    )(
        tokens, query_weight, key_weight, value_weight, output_weight,
        query_gain, key_gain, jnp.asarray(lane_tables(HD)),
        frame_index, row_index, column_index,
    )


def pregather(weight, stride):
    if stride == 1:
        return weight
    count = lax.axis_size("hw")
    groups = [list(range(first, first + stride)) for first in range(0, count, stride)]
    return lax.all_gather(weight, "hw", axis=0, tiled=True, axis_index_groups=groups)


def per_device(
    latents,
    query_weight,
    key_weight,
    value_weight,
    output_weight,
    query_gain,
    key_gain,
    frame_index,
    row_index,
    column_index,
):
    frames, side, width = (latents.shape[1], latents.shape[2], latents.shape[4])
    tokens = latents.reshape(frames * side * side, width)
    grid_columns = lax.axis_size("hw") // DEV_ROWS
    stride = lax.axis_size("hw") // CUBE
    result = attention_block(
        tokens,
        *(pregather(w, stride) for w in (query_weight, key_weight, value_weight, output_weight)),
        query_gain, key_gain, frame_index, row_index, column_index,
        stride, grid_columns, frames, side,
    )
    return result.reshape(1, frames, side, side, output_weight.shape[1])


def solution(mesh):
    placed = (
        P("hw", None, None, None, None),
        P("hw", "head"),
        P("hw", "head"),
        P("hw", "head"),
        P("hw", "head"),
        P("head"),
        P("head"),
        P(),
        P(),
        P(),
    )
    return jax.shard_map(
        per_device,
        mesh=mesh,
        in_specs=placed,
        out_specs=P("hw", None, None, None, "head"),
        check_vma=False,
    )
```
